8 devices in a mesh: batch: 1 (over z), row: 2 (over y), col: 4 (over x, core).
Axes of the slice: x: 2, y: 2, z: 1, core: 2. Of those that a mesh axis runs over, the one named last changes fastest.
Arguments:
- data_mat: bfloat16 [65536, 7168], P(('batch', 'row', 'col'))
- start_block: float32 [7168, 256], P('batch')
Outputs:
- output 1: float32 [7168, 256], P('batch')
- output 2: float32 [256], P('batch')
All inputs are finite; a program needn't handle non-finite values.
Results may differ from the reference program's by a relative error of at most 0.001.
Values are sent between devices in bfloat16 or wider.
A program may use at most 1 GiB of HBM per device.

```python
import jax
import jax.numpy as jnp
from jax import lax

DATA_ROWS = 65536
FEATURES = 7168
SUBSPACE = 256
SWEEPS = 4

ROW_CONTRACT = (((0,), (0,)), ((), ()))


def setup_inputs(seed: int = 0, part: int = 0) -> dict:
    base_key = jax.random.fold_in(jax.random.key(seed), part)
    key_fac, key_load, key_noise, key_start = jax.random.split(base_key, 4)
    levels = 10.0 * 30.0 ** (-jnp.arange(SUBSPACE, dtype=jnp.float32) / (SUBSPACE - 1))
    factors = jax.random.normal(key_fac, (DATA_ROWS, SUBSPACE), jnp.float32)
    loadings = jax.random.normal(key_load, (FEATURES, SUBSPACE), jnp.float32) * jnp.sqrt(levels / FEATURES)[None, :]
    noise_mat = jax.random.normal(key_noise, (DATA_ROWS, FEATURES), jnp.float32) * 0.03 ** 0.5
    data_mat = ((jnp.dot(factors, loadings.T) + noise_mat) * DATA_ROWS ** -0.5).astype(jnp.bfloat16)
    start_block = jax.random.normal(key_start, (FEATURES, SUBSPACE), jnp.float32)
    return {"data_mat": data_mat, "start_block": start_block}


def cholesky_qr2(z_block):
    z_low = z_block.astype(jnp.bfloat16)
    gram_one = lax.dot_general(z_low, z_low, ROW_CONTRACT, preferred_element_type=jnp.float32)
    half_done = lax.linalg.triangular_solve(jnp.linalg.cholesky(gram_one), z_block, left_side=False, lower=True, transpose_a=True)
    gram_two = lax.dot_general(half_done, half_done, ROW_CONTRACT, precision=lax.Precision.HIGHEST, preferred_element_type=jnp.float32)
    return lax.linalg.triangular_solve(jnp.linalg.cholesky(gram_two), half_done, left_side=False, lower=True, transpose_a=True)


def reference(data_mat, start_block):
    def one_sweep(sweep_idx, cur_basis):
        projected = jnp.dot(data_mat, cur_basis.astype(jnp.bfloat16), preferred_element_type=jnp.float32).astype(jnp.bfloat16)
        pulled = lax.dot_general(data_mat, projected, ROW_CONTRACT, preferred_element_type=jnp.float32)
        return cholesky_qr2(pulled)

    q_basis = lax.fori_loop(0, SWEEPS, one_sweep, start_block)
    final_proj = jnp.dot(data_mat, q_basis.astype(jnp.bfloat16), preferred_element_type=jnp.float32)
    ritz_vals = jnp.sum(final_proj * final_proj, axis=0)
    return q_basis, ritz_vals
```

```python
import jax
import jax.numpy as jnp
from jax import lax
from jax.experimental import pallas as pl
from jax.experimental.pallas import tpu as pltpu
from jax.sharding import PartitionSpec as P

SWEEPS = 4
GROUP_AXES = ("row", "col")
ROW_CONTRACT = (((0,), (0,)), ((), ()))
LANE_CONTRACT = (((1,), (1,)), ((), ()))
PLAIN = (((1,), (0,)), ((), ()))
MESH = pl.DeviceIdType.MESH
HALF = 128
PEERS = 7
VMEM_BYTES = 60 * 1024 * 1024


def exact_dot(left, right, dims):
    return lax.dot_general(left, right, dims, precision=lax.Precision.HIGHEST, preferred_element_type=jnp.float32)


def invert_factor(block):
    lane = lax.broadcasted_iota(jnp.int32, (8, HALF), 1)
    sub = lax.broadcasted_iota(jnp.int32, (8, HALF), 0)
    for step in range(HALF // 8):
        base = 8 * step
        inside = (lane >= base) & (lane < base + 8)
        pivots = block[base:base + 8, :]
        cols = [jnp.broadcast_to(pivots[:, base + p:base + p + 1], (8, HALF)) for p in range(8)]
        low = jnp.where(inside, jnp.where(lane - base == sub, 1.0, 0.0), pivots)
        full = low
        scale = jnp.zeros((8, HALF), jnp.float32)
        inverse = jnp.zeros((8, HALF), jnp.float32)
        for p in range(8):
            root = lax.rsqrt(jnp.broadcast_to(cols[p][p:p + 1, :], (8, HALF)))
            recip = root * root
            here = sub == p
            scale = jnp.where(here, root, scale)
            inverse = jnp.where(here, recip, inverse)
            mult = jnp.where(here, 0.0, cols[p] * recip)
            for q in range(p + 1, 8):
                cols[q] = cols[q] - mult * jnp.broadcast_to(cols[q][p:p + 1, :], (8, HALF))
            full_row = jnp.broadcast_to(full[p:p + 1, :], (8, HALF))
            low_row = jnp.broadcast_to(low[p:p + 1, :], (8, HALF))
            full = full - mult * full_row
            low = low - jnp.where(sub > p, mult, 0.0) * low_row
        block[base:base + 8, :] = low * scale
        full = full * inverse
        rows = [jnp.broadcast_to(full[p:p + 1, :], (8, HALF)) for p in range(8)]
        for i in range(step + 1, HALF // 8):
            held = block[8 * i:8 * i + 8, :]
            acc = jnp.where(inside, 0.0, held)
            for p in range(8):
                acc = acc - jnp.broadcast_to(held[:, base + p:base + p + 1], (8, HALF)) * rows[p]
            block[8 * i:8 * i + 8, :] = acc


def factor_inverse(gram, work, inv_low):
    tri = lax.broadcasted_iota(jnp.int32, (HALF, HALF), 0) >= lax.broadcasted_iota(jnp.int32, (HALF, HALF), 1)
    inv_low[:HALF, HALF:] = jnp.zeros((HALF, HALF), jnp.float32)

    @pl.loop(0, 2)
    def _(half):
        @pl.when(half == 0)
        def _():
            work[...] = gram[0:HALF, :]

        @pl.when(half == 1)
        def _():
            upper = exact_dot(inv_low[:HALF, :HALF], gram[HALF:2 * HALF, :], PLAIN)
            work[...] = gram[2 * HALF:3 * HALF, :] - exact_dot(upper, upper, ROW_CONTRACT)
            inv_low[HALF:, :HALF] = exact_dot(upper, inv_low[:HALF, :HALF], ROW_CONTRACT)

        invert_factor(work)
        block_inv = jnp.where(tri, work[...], 0.0)

        @pl.when(half == 0)
        def _():
            inv_low[:HALF, :HALF] = block_inv

        @pl.when(half == 1)
        def _():
            inv_low[HALF:, HALF:] = block_inv
            inv_low[HALF:, :HALF] = -exact_dot(block_inv, inv_low[HALF:, :HALF], PLAIN)


def qr_kernel(z_ref, q_ref, all_ref, part, slots, gram, work, inv_low, sum_send, sum_recv, out_send, out_recv, cast_send, cast_recv):
    row, col = lax.axis_index("row"), lax.axis_index("col")
    me = row * 4 + col
    chunk = 3 * HALF // 8
    rows = z_ref.shape[0]

    def peer(offset):
        other = lax.rem(me + offset, 8)
        return (0, other // 4, lax.rem(other, 4)), other

    barrier = pltpu.get_barrier_semaphore()
    for offset in range(1, 8):
        pl.semaphore_signal(barrier, inc=1, device_id=peer(offset)[0], device_id_type=MESH)
    pl.semaphore_wait(barrier, PEERS)

    def share_gram(turn):
        mine = pl.ds(pl.multiple_of(me * chunk, 8), chunk)
        copies = []
        for offset in range(1, 8):
            device, other = peer(offset)
            copy = pltpu.make_async_remote_copy(
                src_ref=part.at[turn, pl.ds(pl.multiple_of(other * chunk, 8), chunk)],
                dst_ref=slots.at[turn, offset - 1],
                send_sem=sum_send.at[turn, offset - 1],
                recv_sem=sum_recv.at[turn, offset - 1],
                device_id=device,
                device_id_type=MESH,
            )
            copy.start()
            copies.append(copy)
        total = part[turn, mine, :]
        for offset in range(1, 8):
            copies[offset - 1].wait_recv()
            total = total + slots[turn, offset - 1]
        gram[turn, mine, :] = total
        spread = []
        for offset in range(1, 8):
            copy = pltpu.make_async_remote_copy(
                src_ref=gram.at[turn, mine],
                dst_ref=gram.at[turn, mine],
                send_sem=out_send.at[turn, offset - 1],
                recv_sem=out_recv.at[turn, offset - 1],
                device_id=peer(offset)[0],
                device_id_type=MESH,
            )
            copy.start()
            spread.append(copy)
        for copy in copies:
            copy.wait_send()
        for copy in spread:
            copy.wait()

    z_left, z_right = z_ref[:, :HALF].astype(jnp.bfloat16), z_ref[:, HALF:].astype(jnp.bfloat16)
    for place, (left, right) in enumerate(((z_left, z_left), (z_left, z_right), (z_right, z_right))):
        part[0, HALF * place:HALF * (place + 1), :] = lax.dot_general(left, right, ROW_CONTRACT, preferred_element_type=jnp.float32)

    q_ref[...] = z_ref[...]

    def turn_body(turn):
        share_gram(turn)
        factor_inverse(gram.at[turn], work, inv_low)

        @pl.loop(0, rows // HALF)
        def _(i):
            block = pl.ds(pl.multiple_of(i * HALF, HALF), HALF)
            q_ref[block, :] = exact_dot(q_ref[block, :], inv_low[...], LANE_CONTRACT)

        @pl.when(turn == 0)
        def _():
            for place, (left, right) in enumerate(((0, 0), (0, HALF), (HALF, HALF))):
                part[1, HALF * place:HALF * (place + 1), :] = exact_dot(q_ref[:, left:left + HALF], q_ref[:, right:right + HALF], ROW_CONTRACT)

    pl.loop(0, 2)(turn_body)

    core, x = lax.rem(col, 2), col // 2
    twin, x_side, y_side = (0, row, col + 1 - 2 * core), (0, row, core + 2 * (1 - x)), (0, 1 - row, col)
    x_index, y_index, far_index = row * 4 + x_side[2], (1 - row) * 4 + col, (1 - row) * 4 + x_side[2]
    upper, lower = pl.ds(0, rows // 2), pl.ds(rows // 2, rows // 2)
    whole = pl.ds(0, rows)
    all_ref[me] = q_ref[...].astype(jnp.bfloat16)

    def hand(slot, owner, piece, device):
        copy = pltpu.make_async_remote_copy(
            src_ref=all_ref.at[owner, piece],
            dst_ref=all_ref.at[owner, piece],
            send_sem=cast_send.at[slot],
            recv_sem=cast_recv.at[slot],
            device_id=device,
            device_id_type=MESH,
        )
        copy.start()
        return copy

    from_x = hand(0, me, whole, x_side)
    from_y = hand(1, me, whole, y_side)
    from_twin = hand(2, me, whole, twin)
    from_x.wait_recv()
    far_y = hand(3, x_index, upper, y_side)
    twin_x = hand(4, x_index, whole, twin)
    from_y.wait_recv()
    far_x = hand(5, y_index, lower, x_side)
    twin_y = hand(6, y_index, whole, twin)
    far_y.wait_recv()
    far_x.wait_recv()
    twin_far = hand(7, far_index, whole, twin)
    for copy in (from_twin, twin_x, twin_y, twin_far):
        copy.wait_recv()
    for copy in (from_x, from_y, from_twin, far_y, far_x, twin_x, twin_y, twin_far):
        copy.wait_send()


def orthonormalize(z_rows):
    rows, width = z_rows.shape
    return pl.pallas_call(
        qr_kernel,
        out_shape=(jax.ShapeDtypeStruct((rows, width), jnp.float32), jax.ShapeDtypeStruct((8, rows, width), jnp.bfloat16)),
        in_specs=[pl.BlockSpec(memory_space=pltpu.VMEM)],
        out_specs=(pl.BlockSpec(memory_space=pltpu.VMEM), pl.BlockSpec(memory_space=pltpu.VMEM)),
        scratch_shapes=[
            pltpu.VMEM((2, 3 * HALF, HALF), jnp.float32),
            pltpu.VMEM((2, PEERS, 3 * HALF // 8, HALF), jnp.float32),
            pltpu.VMEM((2, 3 * HALF, HALF), jnp.float32),
            pltpu.VMEM((HALF, HALF), jnp.float32),
            pltpu.VMEM((2 * HALF, 2 * HALF), jnp.float32),
            pltpu.SemaphoreType.DMA((2, PEERS)),
            pltpu.SemaphoreType.DMA((2, PEERS)),
            pltpu.SemaphoreType.DMA((2, PEERS)),
            pltpu.SemaphoreType.DMA((2, PEERS)),
            pltpu.SemaphoreType.DMA((8,)),
            pltpu.SemaphoreType.DMA((8,)),
        ],
        compiler_params=pltpu.CompilerParams(collective_id=0, has_side_effects=True),
        cost_estimate=pl.CostEstimate(flops=4 * 10**9, bytes_accessed=6 * 10**6, transcendentals=0),
        name="orthonormalize",
    )(z_rows)


def solution(mesh):
    def device_sweeps(data_local, start_block):
        basis_low = start_block.astype(jnp.bfloat16)
        for _ in range(SWEEPS):
            projected = jnp.dot(data_local, basis_low, preferred_element_type=jnp.float32).astype(jnp.bfloat16)
            pulled_part = lax.dot_general(data_local, projected, ROW_CONTRACT, preferred_element_type=jnp.float32)
            pulled_rows = lax.psum_scatter(pulled_part, GROUP_AXES, scatter_dimension=0, tiled=True)
            q_rows, basis_blocks = orthonormalize(pulled_rows)
            basis_low = basis_blocks.reshape(start_block.shape)
        q_basis = lax.all_gather(q_rows, GROUP_AXES, axis=0, tiled=True)
        final_proj = jnp.dot(data_local, basis_low, preferred_element_type=jnp.float32)
        ritz_vals = lax.psum(jnp.sum(final_proj * final_proj, axis=0), GROUP_AXES)
        return q_basis, ritz_vals

    return jax.shard_map(device_sweeps, mesh=mesh, in_specs=(P(("batch", "row", "col"), None), P("batch", None)), out_specs=(P("batch", None), P("batch")), check_vma=False)
```

```python
import jax
import jax.numpy as jnp
from jax import lax
from jax.experimental import pallas as pl
from jax.experimental.pallas import tpu as pltpu
from jax.sharding import PartitionSpec as P

SWEEPS = 4
GROUP_AXES = ("row", "col")
ROW_CONTRACT = (((0,), (0,)), ((), ()))
LANE_CONTRACT = (((1,), (1,)), ((), ()))
PLAIN = (((1,), (0,)), ((), ()))
MESH = pl.DeviceIdType.MESH
HALF = 128
PEERS = 7
VMEM_BYTES = 63 * 1024 * 1024
TILES = 8
DEPTH = 6


def exact_dot(left, right, dims):
    return lax.dot_general(left, right, dims, precision=lax.Precision.HIGHEST, preferred_element_type=jnp.float32)


def invert_factor(block):
    lane = lax.broadcasted_iota(jnp.int32, (8, HALF), 1)
    sub = lax.broadcasted_iota(jnp.int32, (8, HALF), 0)
    for step in range(HALF // 8):
        base = 8 * step
        inside = (lane >= base) & (lane < base + 8)
        pivots = block[base:base + 8, :]
        cols = [jnp.broadcast_to(pivots[:, base + p:base + p + 1], (8, HALF)) for p in range(8)]
        low = jnp.where(inside, jnp.where(lane - base == sub, 1.0, 0.0), pivots)
        full = low
        scale = jnp.zeros((8, HALF), jnp.float32)
        inverse = jnp.zeros((8, HALF), jnp.float32)
        for p in range(8):
            root = lax.rsqrt(jnp.broadcast_to(cols[p][p:p + 1, :], (8, HALF)))
            recip = root * root
            here = sub == p
            scale = jnp.where(here, root, scale)
            inverse = jnp.where(here, recip, inverse)
            mult = jnp.where(here, 0.0, cols[p] * recip)
            for q in range(p + 1, 8):
                cols[q] = cols[q] - mult * jnp.broadcast_to(cols[q][p:p + 1, :], (8, HALF))
            full_row = jnp.broadcast_to(full[p:p + 1, :], (8, HALF))
            low_row = jnp.broadcast_to(low[p:p + 1, :], (8, HALF))
            full = full - mult * full_row
            low = low - jnp.where(sub > p, mult, 0.0) * low_row
        block[base:base + 8, :] = low * scale
        full = full * inverse
        rows = [jnp.broadcast_to(full[p:p + 1, :], (8, HALF)) for p in range(8)]
        for i in range(step + 1, HALF // 8):
            held = block[8 * i:8 * i + 8, :]
            acc = jnp.where(inside, 0.0, held)
            for p in range(8):
                acc = acc - jnp.broadcast_to(held[:, base + p:base + p + 1], (8, HALF)) * rows[p]
            block[8 * i:8 * i + 8, :] = acc


def factor_inverse(gram, work, inv_low):
    tri = lax.broadcasted_iota(jnp.int32, (HALF, HALF), 0) >= lax.broadcasted_iota(jnp.int32, (HALF, HALF), 1)
    inv_low[:HALF, HALF:] = jnp.zeros((HALF, HALF), jnp.float32)

    @pl.loop(0, 2)
    def _(half):
        @pl.when(half == 0)
        def _():
            work[...] = gram[0:HALF, :]

        @pl.when(half == 1)
        def _():
            upper = exact_dot(inv_low[:HALF, :HALF], gram[HALF:2 * HALF, :], PLAIN)
            work[...] = gram[2 * HALF:3 * HALF, :] - exact_dot(upper, upper, ROW_CONTRACT)
            inv_low[HALF:, :HALF] = exact_dot(upper, inv_low[:HALF, :HALF], ROW_CONTRACT)

        invert_factor(work)
        block_inv = jnp.where(tri, work[...], 0.0)

        @pl.when(half == 0)
        def _():
            inv_low[:HALF, :HALF] = block_inv

        @pl.when(half == 1)
        def _():
            inv_low[HALF:, HALF:] = block_inv
            inv_low[HALF:, :HALF] = -exact_dot(block_inv, inv_low[HALF:, :HALF], PLAIN)


def sweep_kernel(data, basis, z_ref, ring, acc, proj_t, part, from_twin, from_far, from_side, ring_sem, twin_sem, far_sem, side_sem):
    row, col = lax.axis_index("row"), lax.axis_index("col")
    core, x = lax.rem(col, 2), col // 2
    twin, x_side, y_side = (0, row, col + 1 - 2 * core), (0, row, core + 2 * (1 - x)), (0, 1 - row, col)
    tile_rows, chip_cols, width = data.shape[0] // TILES, data.shape[1] // 4, basis.shape[1]
    half, top = chip_cols // 2, width // 2
    turns = 4 * TILES
    skip = turns - DEPTH - 3 * TILES

    def flip(bit, change):
        return bit + change - 2 * bit * change

    def chip_of(step):
        return flip(row, step // 2) * 2 + flip(x, lax.rem(step, 2))

    def fetch(turn, slot):
        first = turn < turns
        local = jnp.where(first, turn, turn - turns)
        step = jnp.where(first, local // TILES, 3 - local // TILES)
        place = jnp.where(first, lax.rem(local, TILES), lax.rem(local + skip, TILES))
        rows = pl.ds(pl.multiple_of(place * tile_rows, tile_rows), tile_rows)
        cols = pl.ds(pl.multiple_of(chip_of(step) * chip_cols, chip_cols), chip_cols)
        return pltpu.make_async_copy(data.at[rows, cols], ring.at[slot], ring_sem.at[slot])

    for turn in range(DEPTH):
        fetch(turn, turn).start()
    acc[...] = jnp.zeros_like(acc)
    part[...] = jnp.zeros_like(part)

    barrier = pltpu.get_barrier_semaphore()
    for device in (twin, x_side, y_side):
        pl.semaphore_signal(barrier, inc=1, device_id=device, device_id_type=MESH)
    pl.semaphore_wait(barrier, 3)

    @pl.loop(0, turns)
    def _(turn):
        slot = lax.rem(turn, DEPTH)
        fetch(turn, slot).wait()
        place = lax.rem(turn, TILES)
        factor = pl.ds(pl.multiple_of(chip_of(turn // TILES) * chip_cols, chip_cols), chip_cols)

        @pl.loop(0, 2)
        def _(piece):
            inner = pl.ds(pl.multiple_of(piece * (tile_rows // 2), tile_rows // 2), tile_rows // 2)
            rows = pl.ds(pl.multiple_of(place * tile_rows + piece * (tile_rows // 2), tile_rows // 2), tile_rows // 2)
            acc[rows, :] += jnp.dot(ring[slot, inner, :], basis[factor, :], preferred_element_type=jnp.float32)

        @pl.when(turn + DEPTH < turns)
        def _():
            fetch(turn + DEPTH, slot).start()

        @pl.when(turn >= 3 * TILES)
        def _():
            rows = pl.ds(pl.multiple_of(place * tile_rows, tile_rows), tile_rows)
            proj_t[place] = acc[rows, :].astype(jnp.bfloat16).T

    mine, other = pl.ds(pl.multiple_of(core * half, HALF), half), pl.ds(pl.multiple_of((1 - core) * half, HALF), half)
    upper, lower = pl.ds(0, top), pl.ds(top, width - top)

    def swap(chunk):
        return pltpu.make_async_remote_copy(
            src_ref=part.at[chunk, :, other], dst_ref=from_twin.at[chunk], send_sem=twin_sem.at[0, chunk], recv_sem=twin_sem.at[1, chunk], device_id=twin, device_id_type=MESH
        )

    def lift(chunk):
        swap(chunk).wait_recv()
        part[chunk, :, mine] = part[chunk, :, mine] + from_twin[chunk]

    def relay(piece, which, device):
        return pltpu.make_async_remote_copy(
            src_ref=part.at[0, piece, mine], dst_ref=from_far.at[which], send_sem=far_sem.at[0, which], recv_sem=far_sem.at[1, which], device_id=device, device_id_type=MESH
        )

    def deliver(chunk, piece, which, device):
        return pltpu.make_async_remote_copy(
            src_ref=part.at[chunk, piece, mine], dst_ref=from_side.at[chunk - 1, piece], send_sem=side_sem.at[0, chunk - 1, which], recv_sem=side_sem.at[1, chunk - 1, which], device_id=device, device_id_type=MESH
        )

    far_to_x, far_to_y = relay(upper, 0, x_side), relay(lower, 1, y_side)
    y_low, y_up = deliver(1, lower, 1, y_side), deliver(1, upper, 0, y_side)
    x_up, x_low = deliver(2, upper, 0, x_side), deliver(2, lower, 1, x_side)

    @pl.loop(0, turns)
    def _(turn):
        slot = lax.rem(turn + turns, DEPTH)

        @pl.when(turn >= DEPTH)
        def _():
            fetch(turn + turns, slot).wait()

        chunk, place = turn // TILES, lax.rem(turn + skip, TILES)
        part[chunk] += jnp.dot(proj_t[place], ring[slot], preferred_element_type=jnp.float32)

        @pl.when(turn + DEPTH < turns)
        def _():
            fetch(turn + turns + DEPTH, slot).start()

        @pl.when(lax.rem(turn, TILES) == TILES - 1)
        def _():
            swap(chunk).start()

        @pl.when(turn == TILES + 1)
        def _():
            lift(0)
            far_to_x.start()
            far_to_y.start()

        @pl.when(turn == 2 * TILES + 1)
        def _():
            lift(1)
            y_low.start()

        @pl.when(turn == 2 * TILES + 5)
        def _():
            far_to_x.wait_recv()
            part[1, upper, mine] = part[1, upper, mine] + from_far[0]
            y_up.start()

        @pl.when(turn == 3 * TILES + 1)
        def _():
            lift(2)
            x_up.start()
            far_to_y.wait_recv()
            part[2, lower, mine] = part[2, lower, mine] + from_far[1]
            x_low.start()

    lift(3)
    y_low.wait_recv()
    y_up.wait_recv()
    z_ref[...] = part[3, :, mine] + from_side[0]
    x_up.wait_recv()
    x_low.wait_recv()
    z_ref[...] += from_side[1]
    for chunk in range(4):
        swap(chunk).wait_send()
    for copy in (far_to_x, far_to_y, y_low, y_up, x_up, x_low):
        copy.wait_send()


def pull_rows(data_local, basis_low):
    rows, features = data_local.shape
    width = basis_low.shape[1]
    tile_rows, chip_cols = rows // TILES, features // 4
    half = chip_cols // 2
    flops = 4 * rows * features * width
    return pl.pallas_call(
        sweep_kernel,
        out_shape=jax.ShapeDtypeStruct((width, half), jnp.float32),
        in_specs=[pl.BlockSpec(memory_space=pl.ANY), pl.BlockSpec(memory_space=pltpu.VMEM)],
        out_specs=pl.BlockSpec(memory_space=pltpu.VMEM),
        scratch_shapes=[
            pltpu.VMEM((DEPTH, tile_rows, chip_cols), jnp.bfloat16),
            pltpu.VMEM((rows, width), jnp.float32),
            pltpu.VMEM((TILES, width, tile_rows), jnp.bfloat16),
            pltpu.VMEM((4, width, chip_cols), jnp.float32),
            pltpu.VMEM((4, width, half), jnp.float32),
            pltpu.VMEM((2, width // 2, half), jnp.float32),
            pltpu.VMEM((2, width, half), jnp.float32),
            pltpu.SemaphoreType.DMA((DEPTH,)),
            pltpu.SemaphoreType.DMA((2, 4)),
            pltpu.SemaphoreType.DMA((2, 2)),
            pltpu.SemaphoreType.DMA((2, 2, 2)),
        ],
        compiler_params=pltpu.CompilerParams(collective_id=1, has_side_effects=True, vmem_limit_bytes=VMEM_BYTES),
        cost_estimate=pl.CostEstimate(flops=flops, bytes_accessed=4 * rows * features, transcendentals=0),
        name="pull_rows",
    )(data_local, basis_low)


def qr_kernel(z_ref, q_ref, all_ref, turned, part, slots, gram, work, inv_low, sum_send, sum_recv, out_send, out_recv, cast_send, cast_recv):
    row, col = lax.axis_index("row"), lax.axis_index("col")
    me = row * 4 + col
    chunk = 3 * HALF // 8
    rows = z_ref.shape[1]

    def peer(offset):
        other = lax.rem(me + offset, 8)
        return (0, other // 4, lax.rem(other, 4)), other

    barrier = pltpu.get_barrier_semaphore()
    for offset in range(1, 8):
        pl.semaphore_signal(barrier, inc=1, device_id=peer(offset)[0], device_id_type=MESH)
    pl.semaphore_wait(barrier, PEERS)

    def share_gram(turn):
        mine = pl.ds(pl.multiple_of(me * chunk, 8), chunk)
        copies = []
        for offset in range(1, 8):
            device, other = peer(offset)
            copy = pltpu.make_async_remote_copy(
                src_ref=part.at[turn, pl.ds(pl.multiple_of(other * chunk, 8), chunk)],
                dst_ref=slots.at[turn, offset - 1],
                send_sem=sum_send.at[turn, offset - 1],
                recv_sem=sum_recv.at[turn, offset - 1],
                device_id=device,
                device_id_type=MESH,
            )
            copy.start()
            copies.append(copy)
        total = part[turn, mine, :]
        for offset in range(1, 8):
            copies[offset - 1].wait_recv()
            total = total + slots[turn, offset - 1]
        gram[turn, mine, :] = total
        spread = []
        for offset in range(1, 8):
            copy = pltpu.make_async_remote_copy(
                src_ref=gram.at[turn, mine],
                dst_ref=gram.at[turn, mine],
                send_sem=out_send.at[turn, offset - 1],
                recv_sem=out_recv.at[turn, offset - 1],
                device_id=peer(offset)[0],
                device_id_type=MESH,
            )
            copy.start()
            spread.append(copy)
        for copy in copies:
            copy.wait_send()
        for copy in spread:
            copy.wait()

    z_left, z_right = z_ref[:HALF, :].astype(jnp.bfloat16), z_ref[HALF:, :].astype(jnp.bfloat16)
    for place, (left, right) in enumerate(((z_left, z_left), (z_left, z_right), (z_right, z_right))):
        part[0, HALF * place:HALF * (place + 1), :] = lax.dot_general(left, right, LANE_CONTRACT, preferred_element_type=jnp.float32)

    turned[...] = z_ref[...]

    def turn_body(turn):
        share_gram(turn)
        factor_inverse(gram.at[turn], work, inv_low)

        @pl.loop(0, rows // HALF)
        def _(i):
            block = pl.ds(pl.multiple_of(i * HALF, HALF), HALF)
            turned[:, block] = exact_dot(inv_low[...], turned[:, block], PLAIN)

        @pl.when(turn == 0)
        def _():
            for place, (left, right) in enumerate(((0, 0), (0, HALF), (HALF, HALF))):
                part[1, HALF * place:HALF * (place + 1), :] = exact_dot(turned[left:left + HALF, :], turned[right:right + HALF, :], LANE_CONTRACT)

    pl.loop(0, 2)(turn_body)

    core, x = lax.rem(col, 2), col // 2
    twin, x_side, y_side = (0, row, col + 1 - 2 * core), (0, row, core + 2 * (1 - x)), (0, 1 - row, col)
    x_index, y_index, far_index = row * 4 + x_side[2], (1 - row) * 4 + col, (1 - row) * 4 + x_side[2]
    upper, lower = pl.ds(0, rows // 2), pl.ds(rows // 2, rows // 2)
    whole = pl.ds(0, rows)

    @pl.loop(0, rows // HALF)
    def _(i):
        block = pl.ds(pl.multiple_of(i * HALF, HALF), HALF)
        q_ref[block, :] = turned[:, block].T
        all_ref[me, block, :] = q_ref[block, :].astype(jnp.bfloat16)


    def hand(slot, owner, piece, device):
        copy = pltpu.make_async_remote_copy(
            src_ref=all_ref.at[owner, piece],
            dst_ref=all_ref.at[owner, piece],
            send_sem=cast_send.at[slot],
            recv_sem=cast_recv.at[slot],
            device_id=device,
            device_id_type=MESH,
        )
        copy.start()
        return copy

    from_x = hand(0, me, whole, x_side)
    from_y = hand(1, me, whole, y_side)
    from_twin = hand(2, me, whole, twin)
    from_x.wait_recv()
    far_y = hand(3, x_index, upper, y_side)
    twin_x = hand(4, x_index, whole, twin)
    from_y.wait_recv()
    far_x = hand(5, y_index, lower, x_side)
    twin_y = hand(6, y_index, whole, twin)
    far_y.wait_recv()
    far_x.wait_recv()
    twin_far = hand(7, far_index, whole, twin)
    for copy in (from_twin, twin_x, twin_y, twin_far):
        copy.wait_recv()
    for copy in (from_x, from_y, from_twin, far_y, far_x, twin_x, twin_y, twin_far):
        copy.wait_send()


def orthonormalize(z_rows):
    width, rows = z_rows.shape
    return pl.pallas_call(
        qr_kernel,
        out_shape=(jax.ShapeDtypeStruct((rows, width), jnp.float32), jax.ShapeDtypeStruct((8, rows, width), jnp.bfloat16)),
        in_specs=[pl.BlockSpec(memory_space=pltpu.VMEM)],
        out_specs=(pl.BlockSpec(memory_space=pltpu.VMEM), pl.BlockSpec(memory_space=pltpu.VMEM)),
        scratch_shapes=[
            pltpu.VMEM((width, rows), jnp.float32),
            pltpu.VMEM((2, 3 * HALF, HALF), jnp.float32),
            pltpu.VMEM((2, PEERS, 3 * HALF // 8, HALF), jnp.float32),
            pltpu.VMEM((2, 3 * HALF, HALF), jnp.float32),
            pltpu.VMEM((HALF, HALF), jnp.float32),
            pltpu.VMEM((2 * HALF, 2 * HALF), jnp.float32),
            pltpu.SemaphoreType.DMA((2, PEERS)),
            pltpu.SemaphoreType.DMA((2, PEERS)),
            pltpu.SemaphoreType.DMA((2, PEERS)),
            pltpu.SemaphoreType.DMA((2, PEERS)),
            pltpu.SemaphoreType.DMA((8,)),
            pltpu.SemaphoreType.DMA((8,)),
        ],
        compiler_params=pltpu.CompilerParams(collective_id=0, has_side_effects=True),
        cost_estimate=pl.CostEstimate(flops=4 * 10**9, bytes_accessed=6 * 10**6, transcendentals=0),
        name="orthonormalize",
    )(z_rows)


def solution(mesh):
    def device_sweeps(data_local, start_block):
        basis_low = start_block.astype(jnp.bfloat16)
        for _ in range(SWEEPS):
            pulled_rows = pull_rows(data_local, basis_low)
            q_rows, basis_blocks = orthonormalize(pulled_rows)
            basis_low = basis_blocks.reshape(start_block.shape)
        q_basis = lax.all_gather(q_rows, GROUP_AXES, axis=0, tiled=True)
        final_proj = jnp.dot(data_local, basis_low, preferred_element_type=jnp.float32)
        ritz_vals = lax.psum(jnp.sum(final_proj * final_proj, axis=0), GROUP_AXES)
        return q_basis, ritz_vals

    return jax.shard_map(device_sweeps, mesh=mesh, in_specs=(P(("batch", "row", "col"), None), P("batch", None)), out_specs=(P("batch", None), P("batch")), check_vma=False)
```

```python
import jax
import jax.numpy as jnp
from jax import lax
from jax.experimental import pallas as pl
from jax.experimental.pallas import tpu as pltpu
from jax.sharding import PartitionSpec as P

SWEEPS = 4
ROW_CONTRACT = (((0,), (0,)), ((), ()))
LANE_CONTRACT = (((1,), (1,)), ((), ()))
PLAIN = (((1,), (0,)), ((), ()))
MESH = pl.DeviceIdType.MESH
HALF = 128
PEERS = 7
VMEM_BYTES = 63 * 1024 * 1024
TILES = 8
DEPTH = 8


def exact_dot(left, right, dims):
    return lax.dot_general(left, right, dims, precision=lax.Precision.HIGHEST, preferred_element_type=jnp.float32)


def invert_factor(block):
    lane = lax.broadcasted_iota(jnp.int32, (8, HALF), 1)
    sub = lax.broadcasted_iota(jnp.int32, (8, HALF), 0)
    for step in range(HALF // 8):
        base = 8 * step
        inside = (lane >= base) & (lane < base + 8)
        pivots = block[base:base + 8, :]
        cols = [jnp.broadcast_to(pivots[:, base + p:base + p + 1], (8, HALF)) for p in range(8)]
        low = jnp.where(inside, jnp.where(lane - base == sub, 1.0, 0.0), pivots)
        full = low
        scale = jnp.zeros((8, HALF), jnp.float32)
        inverse = jnp.zeros((8, HALF), jnp.float32)
        for p in range(8):
            root = lax.rsqrt(jnp.broadcast_to(cols[p][p:p + 1, :], (8, HALF)))
            recip = root * root
            here = sub == p
            scale = jnp.where(here, root, scale)
            inverse = jnp.where(here, recip, inverse)
            mult = jnp.where(here, 0.0, cols[p] * recip)
            for q in range(p + 1, 8):
                cols[q] = cols[q] - mult * jnp.broadcast_to(cols[q][p:p + 1, :], (8, HALF))
            full_row = jnp.broadcast_to(full[p:p + 1, :], (8, HALF))
            low_row = jnp.broadcast_to(low[p:p + 1, :], (8, HALF))
            full = full - mult * full_row
            low = low - jnp.where(sub > p, mult, 0.0) * low_row
        block[base:base + 8, :] = low * scale
        full = full * inverse
        rows = [jnp.broadcast_to(full[p:p + 1, :], (8, HALF)) for p in range(8)]
        for i in range(step + 1, HALF // 8):
            held = block[8 * i:8 * i + 8, :]
            acc = jnp.where(inside, 0.0, held)
            for p in range(8):
                acc = acc - jnp.broadcast_to(held[:, base + p:base + p + 1], (8, HALF)) * rows[p]
            block[8 * i:8 * i + 8, :] = acc


def factor_inverse(gram, work, inv_low):
    tri = lax.broadcasted_iota(jnp.int32, (HALF, HALF), 0) >= lax.broadcasted_iota(jnp.int32, (HALF, HALF), 1)
    inv_low[:HALF, HALF:] = jnp.zeros((HALF, HALF), jnp.float32)

    @pl.loop(0, 2)
    def _(half):
        @pl.when(half == 0)
        def _():
            work[...] = gram[0:HALF, :]

        @pl.when(half == 1)
        def _():
            upper = exact_dot(inv_low[:HALF, :HALF], gram[HALF:2 * HALF, :], PLAIN)
            work[...] = gram[2 * HALF:3 * HALF, :] - exact_dot(upper, upper, ROW_CONTRACT)
            inv_low[HALF:, :HALF] = exact_dot(upper, inv_low[:HALF, :HALF], ROW_CONTRACT)

        invert_factor(work)
        block_inv = jnp.where(tri, work[...], 0.0)

        @pl.when(half == 0)
        def _():
            inv_low[:HALF, :HALF] = block_inv

        @pl.when(half == 1)
        def _():
            inv_low[HALF:, HALF:] = block_inv
            inv_low[HALF:, :HALF] = -exact_dot(block_inv, inv_low[HALF:, :HALF], PLAIN)


def cut_of(chip_cols):
    first = 2 * HALF * ((chip_cols // (2 * HALF) + 1) // 2)
    return first, chip_cols - first


class Place:
    def __init__(self, features):
        self.row, self.col = lax.axis_index("row"), lax.axis_index("col")
        self.core, self.x = lax.rem(self.col, 2), self.col // 2
        self.twin = (0, self.row, self.col + 1 - 2 * self.core)
        self.x_side = (0, self.row, self.core + 2 * (1 - self.x))
        self.y_side = (0, 1 - self.row, self.col)
        self.chip_cols = features // 4
        self.widths = cut_of(self.chip_cols)

    def chip(self, flip_x, flip_y):
        x = self.x + flip_x - 2 * self.x * flip_x
        y = self.row + flip_y - 2 * self.row * flip_y
        return y * 2 + x

    def columns(self, flip_x, flip_y, sub):
        start = self.chip(flip_x, flip_y) * self.chip_cols + sub * self.widths[0]
        return pl.ds(pl.multiple_of(start, 2 * HALF), self.widths[sub])

    def owned(self, flip_x, flip_y, sub):
        start = self.chip(flip_x, flip_y) * self.chip_cols + sub * self.widths[0] + self.core * (self.widths[sub] // 2)
        return pl.ds(pl.multiple_of(start, HALF), self.widths[sub] // 2)


def as_int(flag):
    return jnp.where(flag, 1, 0)


def first_order(block):
    far = block >= 6
    in_x = (block == 2) | (block == 4) | far
    in_y = (block == 3) | (block == 5) | far
    return as_int(in_x), as_int(in_y), as_int((block == 1) | ((block >= 4) & (block <= 6)))


def second_order(block):
    far = block < 2
    in_x = far | (block == 3) | (block == 5)
    in_y = far | (block == 2) | (block == 4)
    return as_int(in_x), as_int(in_y), as_int((block == 1) | (block == 4) | (block == 5) | (block == 7))


def by_width(sub, action):
    for static in range(2):
        pl.when(sub == static)(lambda static=static: action(static))


def tile_copy(place, data, ring, ring_sem, tile, slot, order, begin):
    flip_x, flip_y, sub = order(tile // TILES)
    tile_rows = ring.shape[1]
    rows = pl.ds(pl.multiple_of(lax.rem(tile, TILES) * tile_rows, tile_rows), tile_rows)

    def act(static):
        copy = pltpu.make_async_copy(data.at[rows, place.columns(flip_x, flip_y, static)], ring.at[slot, :, pl.ds(0, place.widths[static])], ring_sem.at[slot])
        copy.start() if begin else copy.wait()

    by_width(sub, act)


def first_pass(place, data, own, landing, basis, ring, acc, ring_sem, gather_sem, clear, finish, after):
    turns = 8 * TILES
    tile_rows = ring.shape[1]
    for turn in range(DEPTH):
        tile_copy(place, data, ring, ring_sem, turn, turn, first_order, True)

    barrier = pltpu.get_barrier_semaphore()
    for offset in range(1, 8):
        other = lax.rem(place.row * 4 + place.col + offset, 8)
        pl.semaphore_signal(barrier, inc=1, device_id=(0, other // 4, lax.rem(other, 4)), device_id_type=MESH)
    pl.semaphore_wait(barrier, PEERS)

    piece = (pl.ds(0, place.widths[0] // 2), pl.ds(place.widths[0] // 2, place.widths[1] // 2))

    def hand(index, flip_x, flip_y, sub, device):
        rows = place.owned(flip_x, flip_y, sub)
        source = own.at[piece[sub]] if flip_x + flip_y == 0 else landing.at[rows]
        return pltpu.make_async_remote_copy(
            src_ref=source, dst_ref=landing.at[rows], send_sem=gather_sem.at[0, index], recv_sem=gather_sem.at[1, index], device_id=device, device_id_type=MESH
        )

    twin, x_side, y_side = place.twin, place.x_side, place.y_side
    copies = [
        hand(0, 0, 0, 0, x_side), hand(1, 0, 0, 0, y_side), hand(2, 0, 0, 0, twin),
        hand(3, 0, 0, 1, x_side), hand(4, 0, 0, 1, y_side), hand(5, 0, 0, 1, twin),
        hand(6, 1, 0, 0, y_side), hand(7, 1, 0, 0, twin), hand(8, 1, 0, 1, twin),
        hand(9, 0, 1, 1, x_side), hand(10, 0, 1, 0, twin), hand(11, 0, 1, 1, twin),
        hand(12, 1, 1, 0, twin), hand(13, 1, 1, 1, twin),
    ]
    for index in range(6):
        copies[index].start()
    for sub in range(2):
        landing[place.owned(0, 0, sub), :] = own[piece[sub], :]
    acc[...] = jnp.zeros_like(acc)
    clear()

    def at(turn, when, waits, starts):
        @pl.when(turn == when)
        def _():
            for index in waits:
                copies[index].wait_recv()
            for index in starts:
                copies[index].start()

    @pl.loop(0, turns)
    def _(turn):
        at(turn, 0, (2,), ())
        at(turn, TILES, (5,), ())
        at(turn, 2 * TILES, (0,), (6, 7))
        at(turn, 2 * TILES, (1,), (10,))
        at(turn, 2 * TILES, (7,), ())
        at(turn, 3 * TILES, (10,), ())
        at(turn, 3 * TILES + 4, (3, 4), (8, 9, 11))
        at(turn, 4 * TILES, (8,), ())
        at(turn, 5 * TILES, (11,), ())
        at(turn, 6 * TILES - 1, (9, 6), (13, 12))
        at(turn, 6 * TILES, (13,), ())
        at(turn, 7 * TILES, (12,), ())
        slot = lax.rem(turn, DEPTH)
        flip_x, flip_y, sub = first_order(turn // TILES)
        tile_copy(place, data, ring, ring_sem, turn, slot, first_order, False)
        part_rows = tile_rows // 2

        def project(static):
            cols = place.columns(flip_x, flip_y, static)
            if landing is not basis:
                @pl.when(lax.rem(turn, TILES) == 0)
                def _():
                    basis[cols, :] = landing[cols, :].astype(jnp.bfloat16)
            for half in range(2):
                inner = pl.ds(half * part_rows, part_rows)
                rows = pl.ds(pl.multiple_of(lax.rem(turn, TILES) * tile_rows + half * part_rows, part_rows), part_rows)
                acc[rows, :] += jnp.dot(ring[slot, inner, pl.ds(0, place.widths[static])], basis[cols, :], preferred_element_type=jnp.float32)

        by_width(sub, project)

        @pl.when(turn + DEPTH < turns)
        def _():
            tile_copy(place, data, ring, ring_sem, turn + DEPTH, slot, first_order, True)

        @pl.when(turn >= turns - TILES)
        def _():
            tile = lax.rem(turn, TILES)
            finish(tile, acc[pl.ds(pl.multiple_of(tile * tile_rows, tile_rows), tile_rows), :])

    after()
    for copy in copies:
        copy.wait_send()


def pull_kernel(data, own, z_ref, basis, ring, acc, proj_t, part0, part1, twin0, twin1, far0, far1, side0, side1, ring_sem, gather_sem, twin_sem, far_sem, side_sem):
    place = Place(data.shape[1])
    twin, x_side, y_side = place.twin, place.x_side, place.y_side
    part, from_twin, from_far, from_side = (part0, part1), (twin0, twin1), (far0, far1), (side0, side1)
    halves = tuple(width // 2 for width in place.widths)
    width = z_ref.shape[0]
    top = width // 2
    turns = 8 * TILES

    def clear():
        part0[...] = jnp.zeros_like(part0)
        part1[...] = jnp.zeros_like(part1)

    def finish(tile, rows):
        proj_t[tile] = rows.astype(jnp.bfloat16).T

    first_pass(place, data, own, basis, basis, ring, acc, ring_sem, gather_sem, clear, finish, lambda: None)

    upper, lower = pl.ds(0, top), pl.ds(top, width - top)
    mine = tuple(pl.ds(pl.multiple_of(place.core * half, HALF), half) for half in halves)
    other = tuple(pl.ds(pl.multiple_of((1 - place.core) * half, HALF), half) for half in halves)
    FAR, Y, X, OWN = 0, 1, 2, 3

    def remote(source, target, sems, device):
        return pltpu.make_async_remote_copy(src_ref=source, dst_ref=target, send_sem=sems.at[0], recv_sem=sems.at[1], device_id=device, device_id_type=MESH)

    swaps, relays, delivers = {}, {}, {}
    for sub in range(2):
        for kind in range(4):
            swaps[kind, sub] = remote(part[sub].at[kind, :, other[sub]], from_twin[sub].at[kind], twin_sem.at[kind, sub], twin)
        relays[0, sub] = remote(part[sub].at[FAR, upper, mine[sub]], from_far[sub].at[0], far_sem.at[0, sub], x_side)
        relays[1, sub] = remote(part[sub].at[FAR, lower, mine[sub]], from_far[sub].at[1], far_sem.at[1, sub], y_side)
        for kind, device in ((Y, y_side), (X, x_side)):
            for which, rows in ((0, upper), (1, lower)):
                delivers[kind, which, sub] = remote(part[sub].at[kind, rows, mine[sub]], from_side[sub].at[kind - 1, rows], side_sem.at[kind - 1, which, sub], device)

    def lift(kind, sub):
        swaps[kind, sub].wait_recv()
        part[sub][kind, :, mine[sub]] = part[sub][kind, :, mine[sub]] + from_twin[sub][kind]

    def send_far(sub):
        lift(FAR, sub)
        relays[0, sub].start()
        relays[1, sub].start()

    def send_side(kind, sub):
        lift(kind, sub)
        plain, joined, rows = (1, 0, upper) if kind == Y else (0, 1, lower)
        delivers[kind, plain, sub].start()
        relays[joined, sub].wait_recv()
        part[sub][kind, rows, mine[sub]] = part[sub][kind, rows, mine[sub]] + from_far[sub][joined]
        delivers[kind, joined, sub].start()

    order = ((FAR, 0), (FAR, 1), (Y, 0), (X, 0), (Y, 1), (X, 1), (OWN, 0), (OWN, 1))

    @pl.loop(0, turns)
    def _(turn):
        slot = lax.rem(turn, DEPTH)
        block, tile = turn // TILES, lax.rem(turn, TILES)
        sub = second_order(block)[2]

        @pl.when(turn >= DEPTH)
        def _():
            tile_copy(place, data, ring, ring_sem, turn, slot, second_order, False)

        kind = jnp.where(block < 2, FAR, jnp.where(block >= 6, OWN, jnp.where((block == 2) | (block == 4), Y, X)))

        def pull(static):
            part[static][kind] += jnp.dot(proj_t[tile], ring[slot, :, pl.ds(0, place.widths[static])], preferred_element_type=jnp.float32)

        by_width(sub, pull)

        @pl.when(turn + DEPTH < turns)
        def _():
            tile_copy(place, data, ring, ring_sem, turn + DEPTH, slot, second_order, True)

        for index, (held, held_sub) in enumerate(order):
            pl.when(turn == (index + 1) * TILES - 1)(lambda held=held, held_sub=held_sub: swaps[held, held_sub].start())
            if held == FAR:
                pl.when(turn == (index + 1) * TILES + 2)(lambda held_sub=held_sub: send_far(held_sub))
            elif held != OWN:
                pl.when(turn == (index + 1) * TILES + 3)(lambda held=held, held_sub=held_sub: send_side(held, held_sub))

    for sub in range(2):
        lanes = pl.ds(sub * halves[0], halves[sub])
        lift(OWN, sub)
        for kind in (Y, X):
            for which in range(2):
                delivers[kind, which, sub].wait_recv()
        z_ref[:, lanes] = (part[sub][OWN, :, mine[sub]] + from_side[sub][0]) + from_side[sub][1]
    for copy in (*swaps.values(), *relays.values(), *delivers.values()):
        copy.wait_send()


def ritz_kernel(data, own, q_ref, r_ref, basis, ring, acc, slots, ring_sem, gather_sem, share_sem):
    place = Place(data.shape[1])
    me = place.row * 4 + place.col
    width = q_ref.shape[1]

    def clear():
        slots[me] = jnp.zeros((8, width), jnp.float32)

    def finish(tile, rows):
        slots[me] += jnp.sum((rows * rows).reshape(rows.shape[0] // 8, 8, width), axis=0)

    def after():
        sends = []
        for offset in range(1, 8):
            other = lax.rem(me + offset, 8)
            copy = pltpu.make_async_remote_copy(
                src_ref=slots.at[me], dst_ref=slots.at[me], send_sem=share_sem.at[0, offset - 1], recv_sem=share_sem.at[1, offset - 1],
                device_id=(0, other // 4, lax.rem(other, 4)), device_id_type=MESH,
            )
            copy.start()
            sends.append(copy)
        for copy in sends:
            copy.wait()
        total = slots[0]
        for index in range(1, 8):
            total = total + slots[index]
        r_ref[...] = jnp.sum(total, axis=0, keepdims=True)

    first_pass(place, data, own, q_ref, basis, ring, acc, ring_sem, gather_sem, clear, finish, after)


def stream_scratch(rows, features, width):
    return [
        pltpu.VMEM((features, width), jnp.bfloat16),
        pltpu.VMEM((DEPTH, rows // TILES, cut_of(features // 4)[0]), jnp.bfloat16),
        pltpu.VMEM((rows, width), jnp.float32),
    ]


def pull_rows(data_local, own):
    rows, features = data_local.shape
    width = own.shape[1]
    widths = cut_of(features // 4)
    pairs = []
    for shape in ((4, width), (4, width), (2, width // 2), (2, width)):
        scale = 1 if not pairs else 2
        pairs += [pltpu.VMEM((*shape, size // scale), jnp.float32) for size in widths]
    return pl.pallas_call(
        pull_kernel,
        out_shape=jax.ShapeDtypeStruct((width, features // 8), jnp.float32),
        in_specs=[pl.BlockSpec(memory_space=pl.ANY), pl.BlockSpec(memory_space=pltpu.VMEM)],
        out_specs=pl.BlockSpec(memory_space=pltpu.VMEM),
        scratch_shapes=[
            *stream_scratch(rows, features, width),
            pltpu.VMEM((TILES, width, rows // TILES), jnp.bfloat16),
            *pairs,
            pltpu.SemaphoreType.DMA((DEPTH,)),
            pltpu.SemaphoreType.DMA((2, 14)),
            pltpu.SemaphoreType.DMA((4, 2, 2)),
            pltpu.SemaphoreType.DMA((2, 2, 2)),
            pltpu.SemaphoreType.DMA((2, 2, 2, 2)),
        ],
        compiler_params=pltpu.CompilerParams(collective_id=1, has_side_effects=True, vmem_limit_bytes=VMEM_BYTES),
        cost_estimate=pl.CostEstimate(flops=4 * rows * features * width, bytes_accessed=4 * rows * features, transcendentals=0),
        name="pull_rows",
    )(data_local, own)


def ritz(data_local, own):
    rows, features = data_local.shape
    width = own.shape[1]
    return pl.pallas_call(
        ritz_kernel,
        out_shape=(jax.ShapeDtypeStruct((features, width), jnp.float32), jax.ShapeDtypeStruct((1, width), jnp.float32)),
        in_specs=[pl.BlockSpec(memory_space=pl.ANY), pl.BlockSpec(memory_space=pltpu.VMEM)],
        out_specs=(pl.BlockSpec(memory_space=pltpu.VMEM), pl.BlockSpec(memory_space=pltpu.VMEM)),
        scratch_shapes=[
            *stream_scratch(rows, features, width),
            pltpu.VMEM((8, 8, width), jnp.float32),
            pltpu.SemaphoreType.DMA((DEPTH,)),
            pltpu.SemaphoreType.DMA((2, 14)),
            pltpu.SemaphoreType.DMA((2, 7)),
        ],
        compiler_params=pltpu.CompilerParams(collective_id=2, has_side_effects=True, vmem_limit_bytes=VMEM_BYTES),
        cost_estimate=pl.CostEstimate(flops=2 * rows * features * width, bytes_accessed=2 * rows * features, transcendentals=0),
        name="ritz",
    )(data_local, own)


def qr_kernel(z_ref, q_ref, low_ref, turned, part, slots, gram, work, inv_low, sum_send, sum_recv, out_send, out_recv):
    row, col = lax.axis_index("row"), lax.axis_index("col")
    me = row * 4 + col
    chunk = 3 * HALF // 8
    rows = z_ref.shape[1]

    def peer(offset):
        other = lax.rem(me + offset, 8)
        return (0, other // 4, lax.rem(other, 4)), other

    barrier = pltpu.get_barrier_semaphore()
    for offset in range(1, 8):
        pl.semaphore_signal(barrier, inc=1, device_id=peer(offset)[0], device_id_type=MESH)
    pl.semaphore_wait(barrier, PEERS)

    def share_gram(turn):
        mine = pl.ds(pl.multiple_of(me * chunk, 8), chunk)
        copies = []
        for offset in range(1, 8):
            device, other = peer(offset)
            copy = pltpu.make_async_remote_copy(
                src_ref=part.at[turn, pl.ds(pl.multiple_of(other * chunk, 8), chunk)],
                dst_ref=slots.at[turn, offset - 1],
                send_sem=sum_send.at[turn, offset - 1],
                recv_sem=sum_recv.at[turn, offset - 1],
                device_id=device,
                device_id_type=MESH,
            )
            copy.start()
            copies.append(copy)
        total = part[turn, mine, :]
        for offset in range(1, 8):
            copies[offset - 1].wait_recv()
            total = total + slots[turn, offset - 1]
        gram[turn, mine, :] = total
        spread = []
        for offset in range(1, 8):
            copy = pltpu.make_async_remote_copy(
                src_ref=gram.at[turn, mine],
                dst_ref=gram.at[turn, mine],
                send_sem=out_send.at[turn, offset - 1],
                recv_sem=out_recv.at[turn, offset - 1],
                device_id=peer(offset)[0],
                device_id_type=MESH,
            )
            copy.start()
            spread.append(copy)
        for copy in copies:
            copy.wait_send()
        for copy in spread:
            copy.wait()

    z_left, z_right = z_ref[:HALF, :].astype(jnp.bfloat16), z_ref[HALF:, :].astype(jnp.bfloat16)
    for place, (left, right) in enumerate(((z_left, z_left), (z_left, z_right), (z_right, z_right))):
        part[0, HALF * place:HALF * (place + 1), :] = lax.dot_general(left, right, LANE_CONTRACT, preferred_element_type=jnp.float32)

    turned[...] = z_ref[...]

    def turn_body(turn):
        share_gram(turn)
        factor_inverse(gram.at[turn], work, inv_low)

        @pl.loop(0, rows // HALF)
        def _(i):
            block = pl.ds(pl.multiple_of(i * HALF, HALF), HALF)
            turned[:, block] = exact_dot(inv_low[...], turned[:, block], PLAIN)

        @pl.when(turn == 0)
        def _():
            for place, (left, right) in enumerate(((0, 0), (0, HALF), (HALF, HALF))):
                part[1, HALF * place:HALF * (place + 1), :] = exact_dot(turned[left:left + HALF, :], turned[right:right + HALF, :], LANE_CONTRACT)

    pl.loop(0, 2)(turn_body)

    @pl.loop(0, rows // HALF)
    def _(i):
        block = pl.ds(pl.multiple_of(i * HALF, HALF), HALF)
        q_ref[block, :] = turned[:, block].T
        low_ref[block, :] = q_ref[block, :].astype(jnp.bfloat16)


def orthonormalize(z_rows):
    width, rows = z_rows.shape
    return pl.pallas_call(
        qr_kernel,
        out_shape=(jax.ShapeDtypeStruct((rows, width), jnp.float32), jax.ShapeDtypeStruct((rows, width), jnp.bfloat16)),
        in_specs=[pl.BlockSpec(memory_space=pltpu.VMEM)],
        out_specs=(pl.BlockSpec(memory_space=pltpu.VMEM), pl.BlockSpec(memory_space=pltpu.VMEM)),
        scratch_shapes=[
            pltpu.VMEM((width, rows), jnp.float32),
            pltpu.VMEM((2, 3 * HALF, HALF), jnp.float32),
            pltpu.VMEM((2, PEERS, 3 * HALF // 8, HALF), jnp.float32),
            pltpu.VMEM((2, 3 * HALF, HALF), jnp.float32),
            pltpu.VMEM((HALF, HALF), jnp.float32),
            pltpu.VMEM((2 * HALF, 2 * HALF), jnp.float32),
            pltpu.SemaphoreType.DMA((2, PEERS)),
            pltpu.SemaphoreType.DMA((2, PEERS)),
            pltpu.SemaphoreType.DMA((2, PEERS)),
            pltpu.SemaphoreType.DMA((2, PEERS)),
        ],
        compiler_params=pltpu.CompilerParams(collective_id=0, has_side_effects=True),
        cost_estimate=pl.CostEstimate(flops=4 * 10**9, bytes_accessed=6 * 10**6, transcendentals=0),
        name="orthonormalize",
    )(z_rows)


def solution(mesh):
    def device_sweeps(data_local, start_block):
        chip_cols = start_block.shape[0] // 4
        row, col = lax.axis_index("row"), lax.axis_index("col")
        first, second = cut_of(chip_cols)
        base, core = (row * 2 + col // 2) * chip_cols, col % 2
        pieces = (lax.dynamic_slice_in_dim(start_block, base + core * (first // 2), first // 2), lax.dynamic_slice_in_dim(start_block, base + first + core * (second // 2), second // 2))
        low_rows = jnp.concatenate(pieces).astype(jnp.bfloat16)
        for _ in range(SWEEPS):
            q_rows, low_rows = orthonormalize(pull_rows(data_local, low_rows))
        q_basis, ritz_vals = ritz(data_local, q_rows)
        return q_basis, ritz_vals.reshape(-1)

    return jax.shard_map(device_sweeps, mesh=mesh, in_specs=(P(("batch", "row", "col"), None), P("batch", None)), out_specs=(P("batch", None), P("batch")), check_vma=False)
```

```python
import jax
import jax.numpy as jnp
from jax import lax
from jax.experimental import pallas as pl
from jax.experimental.pallas import tpu as pltpu
from jax.sharding import PartitionSpec as P

SWEEPS = 4
ROW_CONTRACT = (((0,), (0,)), ((), ()))
LANE_CONTRACT = (((1,), (1,)), ((), ()))
PLAIN = (((1,), (0,)), ((), ()))
MESH = pl.DeviceIdType.MESH
HALF = 128
PEERS = 7
VMEM_BYTES = 63 * 1024 * 1024
TILES = 2
DEPTH = 3
TURNS = 8 * TILES
ROWS_AT_ONCE = 512


def exact_dot(left, right, dims):
    return lax.dot_general(left, right, dims, precision=lax.Precision.HIGHEST, preferred_element_type=jnp.float32)


def invert_factor(block):
    lane = lax.broadcasted_iota(jnp.int32, (8, HALF), 1)
    sub = lax.broadcasted_iota(jnp.int32, (8, HALF), 0)
    for step in range(HALF // 8):
        base = 8 * step
        inside = (lane >= base) & (lane < base + 8)
        pivots = block[base:base + 8, :]
        cols = [jnp.broadcast_to(pivots[:, base + p:base + p + 1], (8, HALF)) for p in range(8)]
        low = jnp.where(inside, jnp.where(lane - base == sub, 1.0, 0.0), pivots)
        full = low
        scale = jnp.zeros((8, HALF), jnp.float32)
        inverse = jnp.zeros((8, HALF), jnp.float32)
        for p in range(8):
            root = lax.rsqrt(jnp.broadcast_to(cols[p][p:p + 1, :], (8, HALF)))
            recip = root * root
            here = sub == p
            scale = jnp.where(here, root, scale)
            inverse = jnp.where(here, recip, inverse)
            mult = jnp.where(here, 0.0, cols[p] * recip)
            for q in range(p + 1, 8):
                cols[q] = cols[q] - mult * jnp.broadcast_to(cols[q][p:p + 1, :], (8, HALF))
            full_row = jnp.broadcast_to(full[p:p + 1, :], (8, HALF))
            low_row = jnp.broadcast_to(low[p:p + 1, :], (8, HALF))
            full = full - mult * full_row
            low = low - jnp.where(sub > p, mult, 0.0) * low_row
        block[base:base + 8, :] = low * scale
        full = full * inverse
        rows = [jnp.broadcast_to(full[p:p + 1, :], (8, HALF)) for p in range(8)]
        for i in range(step + 1, HALF // 8):
            held = block[8 * i:8 * i + 8, :]
            acc = jnp.where(inside, 0.0, held)
            for p in range(8):
                acc = acc - jnp.broadcast_to(held[:, base + p:base + p + 1], (8, HALF)) * rows[p]
            block[8 * i:8 * i + 8, :] = acc


def factor_inverse(gram, work, inv_low):
    tri = lax.broadcasted_iota(jnp.int32, (HALF, HALF), 0) >= lax.broadcasted_iota(jnp.int32, (HALF, HALF), 1)
    inv_low[:HALF, HALF:] = jnp.zeros((HALF, HALF), jnp.float32)

    @pl.loop(0, 2)
    def _(half):
        @pl.when(half == 0)
        def _():
            work[...] = gram[0:HALF, :]

        @pl.when(half == 1)
        def _():
            upper = exact_dot(inv_low[:HALF, :HALF], gram[HALF:2 * HALF, :], PLAIN)
            work[...] = gram[2 * HALF:3 * HALF, :] - exact_dot(upper, upper, ROW_CONTRACT)
            inv_low[HALF:, :HALF] = exact_dot(upper, inv_low[:HALF, :HALF], ROW_CONTRACT)

        invert_factor(work)
        block_inv = jnp.where(tri, work[...], 0.0)

        @pl.when(half == 0)
        def _():
            inv_low[:HALF, :HALF] = block_inv

        @pl.when(half == 1)
        def _():
            inv_low[HALF:, HALF:] = block_inv
            inv_low[HALF:, :HALF] = -exact_dot(block_inv, inv_low[HALF:, :HALF], PLAIN)


def cut_of(chip_cols):
    first = 2 * HALF * ((chip_cols // (2 * HALF) + 1) // 2)
    return first, chip_cols - first


class Place:
    def __init__(self, features):
        self.row, self.col = lax.axis_index("row"), lax.axis_index("col")
        self.core, self.x = lax.rem(self.col, 2), self.col // 2
        self.twin = (0, self.row, self.col + 1 - 2 * self.core)
        self.x_side = (0, self.row, self.core + 2 * (1 - self.x))
        self.y_side = (0, 1 - self.row, self.col)
        self.chip_cols = features // 4
        self.widths = cut_of(self.chip_cols)

    def chip(self, flip_x, flip_y):
        x = self.x + flip_x - 2 * self.x * flip_x
        y = self.row + flip_y - 2 * self.row * flip_y
        return y * 2 + x

    def columns(self, flip_x, flip_y, sub):
        start = self.chip(flip_x, flip_y) * self.chip_cols + sub * self.widths[0]
        return pl.ds(pl.multiple_of(start, 2 * HALF), self.widths[sub])

    def owned(self, flip_x, flip_y, sub):
        start = self.chip(flip_x, flip_y) * self.chip_cols + sub * self.widths[0] + self.core * (self.widths[sub] // 2)
        return pl.ds(pl.multiple_of(start, HALF), self.widths[sub] // 2)


def as_int(flag):
    return jnp.where(flag, 1, 0)


def first_order(block):
    far = block >= 6
    in_x = (block == 2) | (block == 4) | far
    in_y = (block == 3) | (block == 5) | far
    return as_int(in_x), as_int(in_y), as_int((block == 1) | ((block >= 4) & (block <= 6)))


def second_order(block):
    far = block < 2
    in_x = far | (block == 3) | (block == 5)
    in_y = far | (block == 2) | (block == 4)
    return as_int(in_x), as_int(in_y), as_int((block == 1) | (block == 4) | (block == 5) | (block == 7))


def by_width(sub, action):
    for static in range(2):
        pl.when(sub == static)(lambda static=static: action(static))


def tile_copy(place, data, ring, ring_sem, tile, slot, order, begin):
    flip_x, flip_y, sub = order(tile // TILES)
    tile_rows = ring.shape[1]
    rows = pl.ds(pl.multiple_of(lax.rem(tile, TILES) * tile_rows, tile_rows), tile_rows)

    def act(static):
        copy = pltpu.make_async_copy(data.at[rows, place.columns(flip_x, flip_y, static)], ring.at[slot, :, pl.ds(0, place.widths[static])], ring_sem.at[slot])
        copy.start() if begin else copy.wait()

    by_width(sub, act)


def first_pass(place, data, own, landing, basis, ring, acc, ring_sem, gather_sem, second, clear, finish, after):
    turns = TURNS
    tile_rows = ring.shape[1]
    for turn in range(DEPTH):
        tile_copy(place, data, ring, ring_sem, turn, turn, first_order, True)

    barrier = pltpu.get_barrier_semaphore()
    for offset in range(1, 8):
        other = lax.rem(place.row * 4 + place.col + offset, 8)
        pl.semaphore_signal(barrier, inc=1, device_id=(0, other // 4, lax.rem(other, 4)), device_id_type=MESH)
    pl.semaphore_wait(barrier, PEERS)

    piece = (pl.ds(0, place.widths[0] // 2), pl.ds(place.widths[0] // 2, place.widths[1] // 2))

    def hand(index, flip_x, flip_y, sub, device):
        rows = place.owned(flip_x, flip_y, sub)
        source = own.at[piece[sub]] if flip_x + flip_y == 0 else landing.at[rows]
        return pltpu.make_async_remote_copy(
            src_ref=source, dst_ref=landing.at[rows], send_sem=gather_sem.at[0, index], recv_sem=gather_sem.at[1, index], device_id=device, device_id_type=MESH
        )

    twin, x_side, y_side = place.twin, place.x_side, place.y_side
    copies = [
        hand(0, 0, 0, 0, x_side), hand(1, 0, 0, 0, y_side), hand(2, 0, 0, 0, twin),
        hand(3, 0, 0, 1, x_side), hand(4, 0, 0, 1, y_side), hand(5, 0, 0, 1, twin),
        hand(6, 1, 0, 0, y_side), hand(7, 1, 0, 0, twin), hand(8, 1, 0, 1, twin),
        hand(9, 0, 1, 1, x_side), hand(10, 0, 1, 0, twin), hand(11, 0, 1, 1, twin),
        hand(12, 1, 1, 0, twin), hand(13, 1, 1, 1, twin),
    ]
    for index in range(6):
        copies[index].start()
    for sub in range(2):
        landing[place.owned(0, 0, sub), :] = own[piece[sub], :]
    acc[...] = jnp.zeros_like(acc)
    clear()

    def at(turn, when, waits, starts):
        @pl.when(turn == when)
        def _():
            for index in waits:
                copies[index].wait_recv()
            for index in starts:
                copies[index].start()

    @pl.loop(0, turns)
    def _(turn):
        at(turn, 0, (2,), ())
        at(turn, TILES, (5,), ())
        at(turn, 2 * TILES, (0,), (6, 7))
        at(turn, 2 * TILES, (1,), (10,))
        at(turn, 2 * TILES, (7,), ())
        at(turn, 3 * TILES, (10,), ())
        at(turn, 3 * TILES + TILES // 2, (3, 4), (8, 9, 11))
        at(turn, 4 * TILES, (8,), ())
        at(turn, 5 * TILES, (11,), ())
        at(turn, 6 * TILES - 1, (9, 6), (13, 12))
        at(turn, 6 * TILES, (13,), ())
        at(turn, 7 * TILES, (12,), ())
        slot = lax.rem(turn, DEPTH)
        flip_x, flip_y, sub = first_order(turn // TILES)
        tile_copy(place, data, ring, ring_sem, turn, slot, first_order, False)
        part_rows = min(ROWS_AT_ONCE, tile_rows)

        def project(static):
            cols = place.columns(flip_x, flip_y, static)
            if landing is not basis:
                @pl.when(lax.rem(turn, TILES) == 0)
                def _():
                    basis[cols, :] = landing[cols, :].astype(jnp.bfloat16)
            for half in range(tile_rows // part_rows):
                inner = pl.ds(half * part_rows, part_rows)
                rows = pl.ds(pl.multiple_of(lax.rem(turn, TILES) * tile_rows + half * part_rows, part_rows), part_rows)
                acc[rows, :] += jnp.dot(ring[slot, inner, pl.ds(0, place.widths[static])], basis[cols, :], preferred_element_type=jnp.float32)

        by_width(sub, project)

        @pl.when(turn + DEPTH < turns)
        def _():
            tile_copy(place, data, ring, ring_sem, turn + DEPTH, slot, first_order, True)

        if second is not None:
            @pl.when((turn + DEPTH >= turns) & (turn < turns - TILES))
            def _():
                tile_copy(place, data, ring, ring_sem, turn + DEPTH - (turns - TILES), slot, second, True)

        @pl.when(turn >= turns - TILES)
        def _():
            tile = lax.rem(turn, TILES)
            finish(tile, acc[pl.ds(pl.multiple_of(tile * tile_rows, tile_rows), tile_rows), :])

    after()
    for copy in copies:
        copy.wait_send()


def pull_kernel(data, own, z_ref, basis, ring, acc, proj_t, part0, part1, twin0, twin1, far0, far1, side0, side1, ring_sem, gather_sem, twin_sem, far_sem, side_sem):
    place = Place(data.shape[1])
    twin, x_side, y_side = place.twin, place.x_side, place.y_side
    part, from_twin, from_far, from_side = (part0, part1), (twin0, twin1), (far0, far1), (side0, side1)
    halves = tuple(width // 2 for width in place.widths)
    width = z_ref.shape[0]
    top = width // 2
    turns = TURNS

    def clear():
        part0[...] = jnp.zeros_like(part0)
        part1[...] = jnp.zeros_like(part1)

    def finish(tile, rows):
        proj_t[tile] = rows.astype(jnp.bfloat16).T

    first_pass(place, data, own, basis, basis, ring, acc, ring_sem, gather_sem, second_order, clear, finish, lambda: None)

    upper, lower = pl.ds(0, top), pl.ds(top, width - top)
    mine = tuple(pl.ds(pl.multiple_of(place.core * half, HALF), half) for half in halves)
    other = tuple(pl.ds(pl.multiple_of((1 - place.core) * half, HALF), half) for half in halves)
    FAR, Y, X, OWN = 0, 1, 2, 3

    def remote(source, target, sems, device):
        return pltpu.make_async_remote_copy(src_ref=source, dst_ref=target, send_sem=sems.at[0], recv_sem=sems.at[1], device_id=device, device_id_type=MESH)

    swaps, relays, delivers = {}, {}, {}
    for sub in range(2):
        for kind in range(4):
            swaps[kind, sub] = remote(part[sub].at[kind, :, other[sub]], from_twin[sub].at[kind], twin_sem.at[kind, sub], twin)
        relays[0, sub] = remote(part[sub].at[FAR, upper, mine[sub]], from_far[sub].at[0], far_sem.at[0, sub], x_side)
        relays[1, sub] = remote(part[sub].at[FAR, lower, mine[sub]], from_far[sub].at[1], far_sem.at[1, sub], y_side)
        for kind, device in ((Y, y_side), (X, x_side)):
            for which, rows in ((0, upper), (1, lower)):
                delivers[kind, which, sub] = remote(part[sub].at[kind, rows, mine[sub]], from_side[sub].at[kind - 1, rows], side_sem.at[kind - 1, which, sub], device)

    def lift(kind, sub):
        swaps[kind, sub].wait_recv()
        part[sub][kind, :, mine[sub]] = part[sub][kind, :, mine[sub]] + from_twin[sub][kind]

    def send_far(sub):
        lift(FAR, sub)
        relays[0, sub].start()
        relays[1, sub].start()

    def send_side(kind, sub):
        lift(kind, sub)
        plain, joined, rows = (1, 0, upper) if kind == Y else (0, 1, lower)
        delivers[kind, plain, sub].start()
        relays[joined, sub].wait_recv()
        part[sub][kind, rows, mine[sub]] = part[sub][kind, rows, mine[sub]] + from_far[sub][joined]
        delivers[kind, joined, sub].start()

    order = ((FAR, 0), (FAR, 1), (Y, 0), (X, 0), (Y, 1), (X, 1), (OWN, 0), (OWN, 1))

    @pl.loop(0, turns)
    def _(turn):
        slot = lax.rem(turn + turns - TILES, DEPTH)
        block, tile = turn // TILES, lax.rem(turn, TILES)
        sub = second_order(block)[2]

        @pl.when(turn >= TILES)
        def _():
            tile_copy(place, data, ring, ring_sem, turn, slot, second_order, False)

        kind = jnp.where(block < 2, FAR, jnp.where(block >= 6, OWN, jnp.where((block == 2) | (block == 4), Y, X)))

        def pull(static):
            part[static][kind] += jnp.dot(proj_t[tile], ring[slot, :, pl.ds(0, place.widths[static])], preferred_element_type=jnp.float32)

        by_width(sub, pull)

        @pl.when(turn + DEPTH < turns)
        def _():
            tile_copy(place, data, ring, ring_sem, turn + DEPTH, slot, second_order, True)

        for index, (held, held_sub) in enumerate(order):
            pl.when(turn == (index + 1) * TILES - 1)(lambda held=held, held_sub=held_sub: swaps[held, held_sub].start())
            if held == FAR:
                pl.when(turn == (index + 1) * TILES + 0)(lambda held_sub=held_sub: send_far(held_sub))
            elif held != OWN:
                pl.when(turn == (index + 1) * TILES + 0)(lambda held=held, held_sub=held_sub: send_side(held, held_sub))

    for sub in range(2):
        lanes = pl.ds(sub * halves[0], halves[sub])
        lift(OWN, sub)
        for kind in (Y, X):
            for which in range(2):
                delivers[kind, which, sub].wait_recv()
        z_ref[:, lanes] = (part[sub][OWN, :, mine[sub]] + from_side[sub][0]) + from_side[sub][1]
    for copy in (*swaps.values(), *relays.values(), *delivers.values()):
        copy.wait_send()


def ritz_kernel(data, own, q_ref, r_ref, basis, ring, acc, slots, ring_sem, gather_sem, share_sem):
    place = Place(data.shape[1])
    me = place.row * 4 + place.col
    width = q_ref.shape[1]

    def clear():
        slots[me] = jnp.zeros((8, width), jnp.float32)

    def finish(tile, rows):
        slots[me] += jnp.sum((rows * rows).reshape(rows.shape[0] // 8, 8, width), axis=0)

    def after():
        sends = []
        for offset in range(1, 8):
            other = lax.rem(me + offset, 8)
            copy = pltpu.make_async_remote_copy(
                src_ref=slots.at[me], dst_ref=slots.at[me], send_sem=share_sem.at[0, offset - 1], recv_sem=share_sem.at[1, offset - 1],
                device_id=(0, other // 4, lax.rem(other, 4)), device_id_type=MESH,
            )
            copy.start()
            sends.append(copy)
        for copy in sends:
            copy.wait()
        total = slots[0]
        for index in range(1, 8):
            total = total + slots[index]
        r_ref[...] = jnp.sum(total, axis=0, keepdims=True)

    first_pass(place, data, own, q_ref, basis, ring, acc, ring_sem, gather_sem, None, clear, finish, after)


def stream_scratch(rows, features, width):
    return [
        pltpu.VMEM((features, width), jnp.bfloat16),
        pltpu.VMEM((DEPTH, rows // TILES, cut_of(features // 4)[0]), jnp.bfloat16),
        pltpu.VMEM((rows, width), jnp.float32),
    ]


def pull_rows(data_local, own):
    rows, features = data_local.shape
    width = own.shape[1]
    widths = cut_of(features // 4)
    pairs = []
    for shape in ((4, width), (4, width), (2, width // 2), (2, width)):
        scale = 1 if not pairs else 2
        pairs += [pltpu.VMEM((*shape, size // scale), jnp.float32) for size in widths]
    return pl.pallas_call(
        pull_kernel,
        out_shape=jax.ShapeDtypeStruct((width, features // 8), jnp.float32),
        in_specs=[pl.BlockSpec(memory_space=pl.ANY), pl.BlockSpec(memory_space=pltpu.VMEM)],
        out_specs=pl.BlockSpec(memory_space=pltpu.VMEM),
        scratch_shapes=[
            *stream_scratch(rows, features, width),
            pltpu.VMEM((TILES, width, rows // TILES), jnp.bfloat16),
            *pairs,
            pltpu.SemaphoreType.DMA((DEPTH,)),
            pltpu.SemaphoreType.DMA((2, 14)),
            pltpu.SemaphoreType.DMA((4, 2, 2)),
            pltpu.SemaphoreType.DMA((2, 2, 2)),
            pltpu.SemaphoreType.DMA((2, 2, 2, 2)),
        ],
        compiler_params=pltpu.CompilerParams(collective_id=1, has_side_effects=True, vmem_limit_bytes=VMEM_BYTES),
        cost_estimate=pl.CostEstimate(flops=4 * rows * features * width, bytes_accessed=4 * rows * features, transcendentals=0),
        name="pull_rows",
    )(data_local, own)


def ritz(data_local, own):
    rows, features = data_local.shape
    width = own.shape[1]
    return pl.pallas_call(
        ritz_kernel,
        out_shape=(jax.ShapeDtypeStruct((features, width), jnp.float32), jax.ShapeDtypeStruct((1, width), jnp.float32)),
        in_specs=[pl.BlockSpec(memory_space=pl.ANY), pl.BlockSpec(memory_space=pltpu.VMEM)],
        out_specs=(pl.BlockSpec(memory_space=pltpu.VMEM), pl.BlockSpec(memory_space=pltpu.VMEM)),
        scratch_shapes=[
            *stream_scratch(rows, features, width),
            pltpu.VMEM((8, 8, width), jnp.float32),
            pltpu.SemaphoreType.DMA((DEPTH,)),
            pltpu.SemaphoreType.DMA((2, 14)),
            pltpu.SemaphoreType.DMA((2, 7)),
        ],
        compiler_params=pltpu.CompilerParams(collective_id=2, has_side_effects=True, vmem_limit_bytes=VMEM_BYTES),
        cost_estimate=pl.CostEstimate(flops=2 * rows * features * width, bytes_accessed=2 * rows * features, transcendentals=0),
        name="ritz",
    )(data_local, own)


def qr_kernel(z_ref, q_ref, low_ref, turned, part, slots, gram, work, inv_low, sum_send, sum_recv, out_send, out_recv):
    row, col = lax.axis_index("row"), lax.axis_index("col")
    me = row * 4 + col
    chunk = 3 * HALF // 8
    rows = z_ref.shape[1]

    def peer(offset):
        other = lax.rem(me + offset, 8)
        return (0, other // 4, lax.rem(other, 4)), other

    barrier = pltpu.get_barrier_semaphore()
    for offset in range(1, 8):
        pl.semaphore_signal(barrier, inc=1, device_id=peer(offset)[0], device_id_type=MESH)
    pl.semaphore_wait(barrier, PEERS)

    def share_gram(turn):
        mine = pl.ds(pl.multiple_of(me * chunk, 8), chunk)
        copies = []
        for offset in range(1, 8):
            device, other = peer(offset)
            copy = pltpu.make_async_remote_copy(
                src_ref=part.at[turn, pl.ds(pl.multiple_of(other * chunk, 8), chunk)],
                dst_ref=slots.at[turn, offset - 1],
                send_sem=sum_send.at[turn, offset - 1],
                recv_sem=sum_recv.at[turn, offset - 1],
                device_id=device,
                device_id_type=MESH,
            )
            copy.start()
            copies.append(copy)
        total = part[turn, mine, :]
        for offset in range(1, 8):
            copies[offset - 1].wait_recv()
            total = total + slots[turn, offset - 1]
        gram[turn, mine, :] = total
        spread = []
        for offset in range(1, 8):
            copy = pltpu.make_async_remote_copy(
                src_ref=gram.at[turn, mine],
                dst_ref=gram.at[turn, mine],
                send_sem=out_send.at[turn, offset - 1],
                recv_sem=out_recv.at[turn, offset - 1],
                device_id=peer(offset)[0],
                device_id_type=MESH,
            )
            copy.start()
            spread.append(copy)
        for copy in copies:
            copy.wait_send()
        for copy in spread:
            copy.wait()

    z_left, z_right = z_ref[:HALF, :].astype(jnp.bfloat16), z_ref[HALF:, :].astype(jnp.bfloat16)
    for place, (left, right) in enumerate(((z_left, z_left), (z_left, z_right), (z_right, z_right))):
        part[0, HALF * place:HALF * (place + 1), :] = lax.dot_general(left, right, LANE_CONTRACT, preferred_element_type=jnp.float32)

    turned[...] = z_ref[...]

    def turn_body(turn):
        share_gram(turn)
        factor_inverse(gram.at[turn], work, inv_low)

        @pl.loop(0, rows // (2 * HALF))
        def _(i):
            block = pl.ds(pl.multiple_of(i * 2 * HALF, 2 * HALF), 2 * HALF)
            turned[:, block] = exact_dot(inv_low[...], turned[:, block], PLAIN)

        if rows % (2 * HALF):
            rest = pl.ds(rows // (2 * HALF) * 2 * HALF, HALF)
            turned[:, rest] = exact_dot(inv_low[...], turned[:, rest], PLAIN)

        @pl.when(turn == 0)
        def _():
            for place, (left, right) in enumerate(((0, 0), (0, HALF), (HALF, HALF))):
                part[1, HALF * place:HALF * (place + 1), :] = exact_dot(turned[left:left + HALF, :], turned[right:right + HALF, :], LANE_CONTRACT)

    pl.loop(0, 2)(turn_body)

    @pl.loop(0, rows // HALF)
    def _(i):
        block = pl.ds(pl.multiple_of(i * HALF, HALF), HALF)
        q_ref[block, :] = turned[:, block].T
        low_ref[block, :] = q_ref[block, :].astype(jnp.bfloat16)


def orthonormalize(z_rows):
    width, rows = z_rows.shape
    return pl.pallas_call(
        qr_kernel,
        out_shape=(jax.ShapeDtypeStruct((rows, width), jnp.float32), jax.ShapeDtypeStruct((rows, width), jnp.bfloat16)),
        in_specs=[pl.BlockSpec(memory_space=pltpu.VMEM)],
        out_specs=(pl.BlockSpec(memory_space=pltpu.VMEM), pl.BlockSpec(memory_space=pltpu.VMEM)),
        scratch_shapes=[
            pltpu.VMEM((width, rows), jnp.float32),
            pltpu.VMEM((2, 3 * HALF, HALF), jnp.float32),
            pltpu.VMEM((2, PEERS, 3 * HALF // 8, HALF), jnp.float32),
            pltpu.VMEM((2, 3 * HALF, HALF), jnp.float32),
            pltpu.VMEM((HALF, HALF), jnp.float32),
            pltpu.VMEM((2 * HALF, 2 * HALF), jnp.float32),
            pltpu.SemaphoreType.DMA((2, PEERS)),
            pltpu.SemaphoreType.DMA((2, PEERS)),
            pltpu.SemaphoreType.DMA((2, PEERS)),
            pltpu.SemaphoreType.DMA((2, PEERS)),
        ],
        compiler_params=pltpu.CompilerParams(collective_id=0, has_side_effects=True),
        cost_estimate=pl.CostEstimate(flops=4 * 10**9, bytes_accessed=6 * 10**6, transcendentals=0),
        name="orthonormalize",
    )(z_rows)


def solution(mesh):
    def device_sweeps(data_local, start_block):
        chip_cols = start_block.shape[0] // 4
        row, col = lax.axis_index("row"), lax.axis_index("col")
        first, second = cut_of(chip_cols)
        base, core = (row * 2 + col // 2) * chip_cols, col % 2
        pieces = (lax.dynamic_slice_in_dim(start_block, base + core * (first // 2), first // 2), lax.dynamic_slice_in_dim(start_block, base + first + core * (second // 2), second // 2))
        low_rows = jnp.concatenate(pieces).astype(jnp.bfloat16)
        for _ in range(SWEEPS):
            q_rows, low_rows = orthonormalize(pull_rows(data_local, low_rows))
        q_basis, ritz_vals = ritz(data_local, q_rows)
        return q_basis, ritz_vals.reshape(-1)

    return jax.shard_map(device_sweeps, mesh=mesh, in_specs=(P(("batch", "row", "col"), None), P("batch", None)), out_specs=(P("batch", None), P("batch")), check_vma=False)
```

```python
import jax
import jax.numpy as jnp
from jax import lax
from jax.experimental import pallas as pl
from jax.experimental.pallas import tpu as pltpu
from jax.sharding import PartitionSpec as P

SWEEPS = 4
ROW_CONTRACT = (((0,), (0,)), ((), ()))
LANE_CONTRACT = (((1,), (1,)), ((), ()))
PLAIN = (((1,), (0,)), ((), ()))
MESH = pl.DeviceIdType.MESH
HALF = 128
PEERS = 7
VMEM_BYTES = 63 * 1024 * 1024
TILES = 2
DEPTH = 3
TURNS = 8 * TILES
ROWS_AT_ONCE = 512


def exact_dot(left, right, dims):
    return lax.dot_general(left, right, dims, precision=lax.Precision.HIGHEST, preferred_element_type=jnp.float32)


def invert_factor(block):
    lane = lax.broadcasted_iota(jnp.int32, (8, HALF), 1)
    sub = lax.broadcasted_iota(jnp.int32, (8, HALF), 0)
    for step in range(HALF // 8):
        base = 8 * step
        inside = (lane >= base) & (lane < base + 8)
        pivots = block[base:base + 8, :]
        cols = [jnp.broadcast_to(pivots[:, base + p:base + p + 1], (8, HALF)) for p in range(8)]
        low = jnp.where(inside, jnp.where(lane - base == sub, 1.0, 0.0), pivots)
        full = low
        scale = jnp.zeros((8, HALF), jnp.float32)
        inverse = jnp.zeros((8, HALF), jnp.float32)
        for p in range(8):
            root = lax.rsqrt(jnp.broadcast_to(cols[p][p:p + 1, :], (8, HALF)))
            recip = root * root
            here = sub == p
            scale = jnp.where(here, root, scale)
            inverse = jnp.where(here, recip, inverse)
            mult = jnp.where(here, 0.0, cols[p] * recip)
            for q in range(p + 1, 8):
                cols[q] = cols[q] - mult * jnp.broadcast_to(cols[q][p:p + 1, :], (8, HALF))
            full_row = jnp.broadcast_to(full[p:p + 1, :], (8, HALF))
            low_row = jnp.broadcast_to(low[p:p + 1, :], (8, HALF))
            full = full - mult * full_row
            low = low - jnp.where(sub > p, mult, 0.0) * low_row
        block[base:base + 8, :] = low * scale
        full = full * inverse
        rows = [jnp.broadcast_to(full[p:p + 1, :], (8, HALF)) for p in range(8)]
        for i in range(step + 1, HALF // 8):
            held = block[8 * i:8 * i + 8, :]
            acc = jnp.where(inside, 0.0, held)
            for p in range(8):
                acc = acc - jnp.broadcast_to(held[:, base + p:base + p + 1], (8, HALF)) * rows[p]
            block[8 * i:8 * i + 8, :] = acc


def factor_inverse(gram, work, inv_low):
    tri = lax.broadcasted_iota(jnp.int32, (HALF, HALF), 0) >= lax.broadcasted_iota(jnp.int32, (HALF, HALF), 1)
    inv_low[:HALF, HALF:] = jnp.zeros((HALF, HALF), jnp.float32)

    @pl.loop(0, 2)
    def _(half):
        @pl.when(half == 0)
        def _():
            work[...] = gram[0:HALF, :]

        @pl.when(half == 1)
        def _():
            upper = exact_dot(inv_low[:HALF, :HALF], gram[HALF:2 * HALF, :], PLAIN)
            work[...] = gram[2 * HALF:3 * HALF, :] - exact_dot(upper, upper, ROW_CONTRACT)
            inv_low[HALF:, :HALF] = exact_dot(upper, inv_low[:HALF, :HALF], ROW_CONTRACT)

        invert_factor(work)
        block_inv = jnp.where(tri, work[...], 0.0)

        @pl.when(half == 0)
        def _():
            inv_low[:HALF, :HALF] = block_inv

        @pl.when(half == 1)
        def _():
            inv_low[HALF:, HALF:] = block_inv
            inv_low[HALF:, :HALF] = -exact_dot(block_inv, inv_low[HALF:, :HALF], PLAIN)


def orthonormalize(q_ref, low_ref, turned, part, slots, gram, work, inv_low, sum_send, sum_recv, out_send, out_recv):
    row, col = lax.axis_index("row"), lax.axis_index("col")
    me = row * 4 + col
    chunk = 3 * HALF // 8
    rows = turned.shape[1]

    def peer(offset):
        other = lax.rem(me + offset, 8)
        return (0, other // 4, lax.rem(other, 4)), other

    def share_gram(turn):
        mine = pl.ds(pl.multiple_of(me * chunk, 8), chunk)
        copies = []
        for offset in range(1, 8):
            device, other = peer(offset)
            copy = pltpu.make_async_remote_copy(
                src_ref=part.at[turn, pl.ds(pl.multiple_of(other * chunk, 8), chunk)],
                dst_ref=slots.at[turn, offset - 1],
                send_sem=sum_send.at[turn, offset - 1],
                recv_sem=sum_recv.at[turn, offset - 1],
                device_id=device,
                device_id_type=MESH,
            )
            copy.start()
            copies.append(copy)
        total = part[turn, mine, :]
        for offset in range(1, 8):
            copies[offset - 1].wait_recv()
            total = total + slots[turn, offset - 1]
        gram[turn, mine, :] = total
        spread = []
        for offset in range(1, 8):
            copy = pltpu.make_async_remote_copy(
                src_ref=gram.at[turn, mine],
                dst_ref=gram.at[turn, mine],
                send_sem=out_send.at[turn, offset - 1],
                recv_sem=out_recv.at[turn, offset - 1],
                device_id=peer(offset)[0],
                device_id_type=MESH,
            )
            copy.start()
            spread.append(copy)
        for copy in copies:
            copy.wait_send()
        for copy in spread:
            copy.wait()

    z_left, z_right = turned[:HALF, :].astype(jnp.bfloat16), turned[HALF:, :].astype(jnp.bfloat16)
    for place, (left, right) in enumerate(((z_left, z_left), (z_left, z_right), (z_right, z_right))):
        part[0, HALF * place:HALF * (place + 1), :] = lax.dot_general(left, right, LANE_CONTRACT, preferred_element_type=jnp.float32)

    def turn_body(turn):
        share_gram(turn)
        factor_inverse(gram.at[turn], work, inv_low)

        @pl.loop(0, rows // (2 * HALF))
        def _(i):
            block = pl.ds(pl.multiple_of(i * 2 * HALF, 2 * HALF), 2 * HALF)
            turned[:, block] = exact_dot(inv_low[...], turned[:, block], PLAIN)

        if rows % (2 * HALF):
            rest = pl.ds(rows // (2 * HALF) * 2 * HALF, HALF)
            turned[:, rest] = exact_dot(inv_low[...], turned[:, rest], PLAIN)

        @pl.when(turn == 0)
        def _():
            for place, (left, right) in enumerate(((0, 0), (0, HALF), (HALF, HALF))):
                part[1, HALF * place:HALF * (place + 1), :] = exact_dot(turned[left:left + HALF, :], turned[right:right + HALF, :], LANE_CONTRACT)

    pl.loop(0, 2)(turn_body)

    @pl.loop(0, rows // HALF)
    def _(i):
        block = pl.ds(pl.multiple_of(i * HALF, HALF), HALF)
        q_ref[block, :] = turned[:, block].T
        low_ref[block, :] = q_ref[block, :].astype(jnp.bfloat16)


def cut_of(chip_cols):
    first = 2 * HALF * ((chip_cols // (2 * HALF) + 1) // 2)
    return first, chip_cols - first


class Place:
    def __init__(self, features):
        self.row, self.col = lax.axis_index("row"), lax.axis_index("col")
        self.core, self.x = lax.rem(self.col, 2), self.col // 2
        self.twin = (0, self.row, self.col + 1 - 2 * self.core)
        self.x_side = (0, self.row, self.core + 2 * (1 - self.x))
        self.y_side = (0, 1 - self.row, self.col)
        self.chip_cols = features // 4
        self.widths = cut_of(self.chip_cols)

    def chip(self, flip_x, flip_y):
        x = self.x + flip_x - 2 * self.x * flip_x
        y = self.row + flip_y - 2 * self.row * flip_y
        return y * 2 + x

    def columns(self, flip_x, flip_y, sub):
        start = self.chip(flip_x, flip_y) * self.chip_cols + sub * self.widths[0]
        return pl.ds(pl.multiple_of(start, 2 * HALF), self.widths[sub])

    def owned(self, flip_x, flip_y, sub):
        start = self.chip(flip_x, flip_y) * self.chip_cols + sub * self.widths[0] + self.core * (self.widths[sub] // 2)
        return pl.ds(pl.multiple_of(start, HALF), self.widths[sub] // 2)


def as_int(flag):
    return jnp.where(flag, 1, 0)


def first_order(block):
    far = block >= 6
    in_x = (block == 2) | (block == 4) | far
    in_y = (block == 3) | (block == 5) | far
    return as_int(in_x), as_int(in_y), as_int((block == 1) | ((block >= 4) & (block <= 6)))


def second_order(block):
    far = block < 2
    in_x = far | (block == 3) | (block == 5)
    in_y = far | (block == 2) | (block == 4)
    return as_int(in_x), as_int(in_y), as_int((block == 1) | (block == 4) | (block == 5) | (block == 7))


def by_width(sub, action):
    for static in range(2):
        pl.when(sub == static)(lambda static=static: action(static))


def tile_copy(place, data, ring, ring_sem, tile, slot, order, begin):
    flip_x, flip_y, sub = order(tile // TILES)
    tile_rows = ring.shape[1]
    rows = pl.ds(pl.multiple_of(lax.rem(tile, TILES) * tile_rows, tile_rows), tile_rows)

    def act(static):
        copy = pltpu.make_async_copy(data.at[rows, place.columns(flip_x, flip_y, static)], ring.at[slot, :, pl.ds(0, place.widths[static])], ring_sem.at[slot])
        copy.start() if begin else copy.wait()

    by_width(sub, act)


def first_pass(place, data, own, landing, basis, ring, acc, ring_sem, gather_sem, second, clear, finish, after):
    turns = TURNS
    tile_rows = ring.shape[1]
    for turn in range(DEPTH):
        tile_copy(place, data, ring, ring_sem, turn, turn, first_order, True)

    barrier = pltpu.get_barrier_semaphore()
    for offset in range(1, 8):
        other = lax.rem(place.row * 4 + place.col + offset, 8)
        pl.semaphore_signal(barrier, inc=1, device_id=(0, other // 4, lax.rem(other, 4)), device_id_type=MESH)
    pl.semaphore_wait(barrier, PEERS)

    piece = (pl.ds(0, place.widths[0] // 2), pl.ds(place.widths[0] // 2, place.widths[1] // 2))

    def hand(index, flip_x, flip_y, sub, device):
        rows = place.owned(flip_x, flip_y, sub)
        source = own.at[piece[sub]] if flip_x + flip_y == 0 else landing.at[rows]
        return pltpu.make_async_remote_copy(
            src_ref=source, dst_ref=landing.at[rows], send_sem=gather_sem.at[0, index], recv_sem=gather_sem.at[1, index], device_id=device, device_id_type=MESH
        )

    twin, x_side, y_side = place.twin, place.x_side, place.y_side
    copies = [
        hand(0, 0, 0, 0, x_side), hand(1, 0, 0, 0, y_side), hand(2, 0, 0, 0, twin),
        hand(3, 0, 0, 1, x_side), hand(4, 0, 0, 1, y_side), hand(5, 0, 0, 1, twin),
        hand(6, 1, 0, 0, y_side), hand(7, 1, 0, 0, twin), hand(8, 1, 0, 1, twin),
        hand(9, 0, 1, 1, x_side), hand(10, 0, 1, 0, twin), hand(11, 0, 1, 1, twin),
        hand(12, 1, 1, 0, twin), hand(13, 1, 1, 1, twin),
    ]
    for index in range(6):
        copies[index].start()
    for sub in range(2):
        landing[place.owned(0, 0, sub), :] = own[piece[sub], :]
    acc[...] = jnp.zeros_like(acc)
    clear()

    def at(turn, when, waits, starts):
        @pl.when(turn == when)
        def _():
            for index in waits:
                copies[index].wait_recv()
            for index in starts:
                copies[index].start()

    @pl.loop(0, turns)
    def _(turn):
        at(turn, 0, (2,), ())
        at(turn, TILES, (5,), ())
        at(turn, 2 * TILES - 1, (0,), (6, 7))
        at(turn, 2 * TILES - 1, (1,), (10,))
        at(turn, 2 * TILES, (7,), ())
        at(turn, 3 * TILES, (10,), ())
        at(turn, 3 * TILES + TILES // 2, (3, 4), (8, 9, 11))
        at(turn, 4 * TILES, (8,), ())
        at(turn, 5 * TILES, (11,), ())
        at(turn, 6 * TILES - 1, (9, 6), (13, 12))
        at(turn, 6 * TILES, (13,), ())
        at(turn, 7 * TILES, (12,), ())
        slot = lax.rem(turn, DEPTH)
        flip_x, flip_y, sub = first_order(turn // TILES)
        tile_copy(place, data, ring, ring_sem, turn, slot, first_order, False)
        part_rows = min(ROWS_AT_ONCE, tile_rows)

        def project(static):
            cols = place.columns(flip_x, flip_y, static)
            if landing is not basis:
                @pl.when(lax.rem(turn, TILES) == 0)
                def _():
                    basis[cols, :] = landing[cols, :].astype(jnp.bfloat16)
            for half in range(tile_rows // part_rows):
                inner = pl.ds(half * part_rows, part_rows)
                rows = pl.ds(pl.multiple_of(lax.rem(turn, TILES) * tile_rows + half * part_rows, part_rows), part_rows)
                acc[rows, :] += jnp.dot(ring[slot, inner, pl.ds(0, place.widths[static])], basis[cols, :], preferred_element_type=jnp.float32)

        by_width(sub, project)

        @pl.when(turn + DEPTH < turns)
        def _():
            tile_copy(place, data, ring, ring_sem, turn + DEPTH, slot, first_order, True)

        if second is not None:
            @pl.when((turn + DEPTH >= turns) & (turn < turns - TILES))
            def _():
                tile_copy(place, data, ring, ring_sem, turn + DEPTH - (turns - TILES), slot, second, True)

        @pl.when(turn >= turns - TILES)
        def _():
            tile = lax.rem(turn, TILES)
            finish(tile, acc[pl.ds(pl.multiple_of(tile * tile_rows, tile_rows), tile_rows), :])

    after()
    for copy in copies:
        copy.wait_send()


def sweep_kernel(data, own, q_ref, low_ref, turned, gram_part, gram_slots, gram, work, inv_low, sum_send, sum_recv, out_send, out_recv, basis, ring, acc, proj_t, part0, part1, twin0, twin1, far0, far1, side0, side1, ring_sem, gather_sem, twin_sem, far_sem, side_sem):
    place = Place(data.shape[1])
    twin, x_side, y_side = place.twin, place.x_side, place.y_side
    part, from_twin, from_far, from_side = (part0, part1), (twin0, twin1), (far0, far1), (side0, side1)
    halves = tuple(width // 2 for width in place.widths)
    width = turned.shape[0]
    top = width // 2
    turns = TURNS

    def clear():
        part0[...] = jnp.zeros_like(part0)
        part1[...] = jnp.zeros_like(part1)

    def finish(tile, rows):
        proj_t[tile] = rows.astype(jnp.bfloat16).T

    first_pass(place, data, own, basis, basis, ring, acc, ring_sem, gather_sem, second_order, clear, finish, lambda: None)

    upper, lower = pl.ds(0, top), pl.ds(top, width - top)
    mine = tuple(pl.ds(pl.multiple_of(place.core * half, HALF), half) for half in halves)
    other = tuple(pl.ds(pl.multiple_of((1 - place.core) * half, HALF), half) for half in halves)
    FAR, Y, X, OWN = 0, 1, 2, 3

    def remote(source, target, sems, device):
        return pltpu.make_async_remote_copy(src_ref=source, dst_ref=target, send_sem=sems.at[0], recv_sem=sems.at[1], device_id=device, device_id_type=MESH)

    swaps, relays, delivers = {}, {}, {}
    for sub in range(2):
        for kind in range(4):
            swaps[kind, sub] = remote(part[sub].at[kind, :, other[sub]], from_twin[sub].at[kind], twin_sem.at[kind, sub], twin)
        relays[0, sub] = remote(part[sub].at[FAR, upper, mine[sub]], from_far[sub].at[0], far_sem.at[0, sub], x_side)
        relays[1, sub] = remote(part[sub].at[FAR, lower, mine[sub]], from_far[sub].at[1], far_sem.at[1, sub], y_side)
        for kind, device in ((Y, y_side), (X, x_side)):
            for which, rows in ((0, upper), (1, lower)):
                delivers[kind, which, sub] = remote(part[sub].at[kind, rows, mine[sub]], from_side[sub].at[kind - 1, rows], side_sem.at[kind - 1, which, sub], device)

    def lift(kind, sub):
        swaps[kind, sub].wait_recv()
        part[sub][kind, :, mine[sub]] = part[sub][kind, :, mine[sub]] + from_twin[sub][kind]

    def send_far(sub):
        lift(FAR, sub)
        relays[0, sub].start()
        relays[1, sub].start()

    def send_side(kind, sub):
        lift(kind, sub)
        plain, joined, rows = (1, 0, upper) if kind == Y else (0, 1, lower)
        delivers[kind, plain, sub].start()
        relays[joined, sub].wait_recv()
        part[sub][kind, rows, mine[sub]] = part[sub][kind, rows, mine[sub]] + from_far[sub][joined]
        delivers[kind, joined, sub].start()

    order = ((FAR, 0), (FAR, 1), (Y, 0), (X, 0), (Y, 1), (X, 1), (OWN, 0), (OWN, 1))

    @pl.loop(0, turns)
    def _(turn):
        slot = lax.rem(turn + turns - TILES, DEPTH)
        block, tile = turn // TILES, lax.rem(turn, TILES)
        sub = second_order(block)[2]

        @pl.when(turn >= TILES)
        def _():
            tile_copy(place, data, ring, ring_sem, turn, slot, second_order, False)

        kind = jnp.where(block < 2, FAR, jnp.where(block >= 6, OWN, jnp.where((block == 2) | (block == 4), Y, X)))

        def pull(static):
            part[static][kind] += jnp.dot(proj_t[tile], ring[slot, :, pl.ds(0, place.widths[static])], preferred_element_type=jnp.float32)

        by_width(sub, pull)

        @pl.when(turn + DEPTH < turns)
        def _():
            tile_copy(place, data, ring, ring_sem, turn + DEPTH, slot, second_order, True)

        for index, (held, held_sub) in enumerate(order):
            pl.when(turn == (index + 1) * TILES - 1)(lambda held=held, held_sub=held_sub: swaps[held, held_sub].start())
            if held == FAR:
                pl.when(turn == (index + 1) * TILES + 0)(lambda held_sub=held_sub: send_far(held_sub))
            elif held != OWN:
                pl.when(turn == (index + 1) * TILES + 0)(lambda held=held, held_sub=held_sub: send_side(held, held_sub))

    for sub in range(2):
        lanes = pl.ds(sub * halves[0], halves[sub])
        lift(OWN, sub)
        for kind in (Y, X):
            for which in range(2):
                delivers[kind, which, sub].wait_recv()
        turned[:, lanes] = (part[sub][OWN, :, mine[sub]] + from_side[sub][0]) + from_side[sub][1]
    orthonormalize(q_ref, low_ref, turned, gram_part, gram_slots, gram, work, inv_low, sum_send, sum_recv, out_send, out_recv)
    for copy in (*swaps.values(), *relays.values(), *delivers.values()):
        copy.wait_send()


def ritz_kernel(data, own, q_ref, r_ref, basis, ring, acc, slots, ring_sem, gather_sem, share_sem):
    place = Place(data.shape[1])
    me = place.row * 4 + place.col
    width = q_ref.shape[1]

    def clear():
        slots[me] = jnp.zeros((8, width), jnp.float32)

    def finish(tile, rows):
        slots[me] += jnp.sum((rows * rows).reshape(rows.shape[0] // 8, 8, width), axis=0)

    def after():
        sends = []
        for offset in range(1, 8):
            other = lax.rem(me + offset, 8)
            copy = pltpu.make_async_remote_copy(
                src_ref=slots.at[me], dst_ref=slots.at[me], send_sem=share_sem.at[0, offset - 1], recv_sem=share_sem.at[1, offset - 1],
                device_id=(0, other // 4, lax.rem(other, 4)), device_id_type=MESH,
            )
            copy.start()
            sends.append(copy)
        for copy in sends:
            copy.wait()
        total = slots[0]
        for index in range(1, 8):
            total = total + slots[index]
        r_ref[...] = jnp.sum(total, axis=0, keepdims=True)

    first_pass(place, data, own, q_ref, basis, ring, acc, ring_sem, gather_sem, None, clear, finish, after)


def stream_scratch(rows, features, width):
    return [
        pltpu.VMEM((features, width), jnp.bfloat16),
        pltpu.VMEM((DEPTH, rows // TILES, cut_of(features // 4)[0]), jnp.bfloat16),
        pltpu.VMEM((rows, width), jnp.float32),
    ]


def sweep(data_local, own):
    rows, features = data_local.shape
    width = own.shape[1]
    widths = cut_of(features // 4)
    pairs = []
    for shape in ((4, width), (4, width), (2, width // 2), (2, width)):
        scale = 1 if not pairs else 2
        pairs += [pltpu.VMEM((*shape, size // scale), jnp.float32) for size in widths]
    return pl.pallas_call(
        sweep_kernel,
        out_shape=(jax.ShapeDtypeStruct((features // 8, width), jnp.float32), jax.ShapeDtypeStruct((features // 8, width), jnp.bfloat16)),
        in_specs=[pl.BlockSpec(memory_space=pl.ANY), pl.BlockSpec(memory_space=pltpu.VMEM)],
        out_specs=(pl.BlockSpec(memory_space=pltpu.VMEM), pl.BlockSpec(memory_space=pltpu.VMEM)),
        scratch_shapes=[
            pltpu.VMEM((width, features // 8), jnp.float32),
            pltpu.VMEM((2, 3 * HALF, HALF), jnp.float32),
            pltpu.VMEM((2, PEERS, 3 * HALF // 8, HALF), jnp.float32),
            pltpu.VMEM((2, 3 * HALF, HALF), jnp.float32),
            pltpu.VMEM((HALF, HALF), jnp.float32),
            pltpu.VMEM((2 * HALF, 2 * HALF), jnp.float32),
            pltpu.SemaphoreType.DMA((2, PEERS)),
            pltpu.SemaphoreType.DMA((2, PEERS)),
            pltpu.SemaphoreType.DMA((2, PEERS)),
            pltpu.SemaphoreType.DMA((2, PEERS)),
            *stream_scratch(rows, features, width),
            pltpu.VMEM((TILES, width, rows // TILES), jnp.bfloat16),
            *pairs,
            pltpu.SemaphoreType.DMA((DEPTH,)),
            pltpu.SemaphoreType.DMA((2, 14)),
            pltpu.SemaphoreType.DMA((4, 2, 2)),
            pltpu.SemaphoreType.DMA((2, 2, 2)),
            pltpu.SemaphoreType.DMA((2, 2, 2, 2)),
        ],
        compiler_params=pltpu.CompilerParams(collective_id=1, has_side_effects=True, vmem_limit_bytes=VMEM_BYTES),
        cost_estimate=pl.CostEstimate(flops=4 * rows * features * width, bytes_accessed=4 * rows * features, transcendentals=0),
        name="sweep",
    )(data_local, own)


def ritz(data_local, own):
    rows, features = data_local.shape
    width = own.shape[1]
    return pl.pallas_call(
        ritz_kernel,
        out_shape=(jax.ShapeDtypeStruct((features, width), jnp.float32), jax.ShapeDtypeStruct((1, width), jnp.float32)),
        in_specs=[pl.BlockSpec(memory_space=pl.ANY), pl.BlockSpec(memory_space=pltpu.VMEM)],
        out_specs=(pl.BlockSpec(memory_space=pltpu.VMEM), pl.BlockSpec(memory_space=pltpu.VMEM)),
        scratch_shapes=[
            *stream_scratch(rows, features, width),
            pltpu.VMEM((8, 8, width), jnp.float32),
            pltpu.SemaphoreType.DMA((DEPTH,)),
            pltpu.SemaphoreType.DMA((2, 14)),
            pltpu.SemaphoreType.DMA((2, 7)),
        ],
        compiler_params=pltpu.CompilerParams(collective_id=2, has_side_effects=True, vmem_limit_bytes=VMEM_BYTES),
        cost_estimate=pl.CostEstimate(flops=2 * rows * features * width, bytes_accessed=2 * rows * features, transcendentals=0),
        name="ritz",
    )(data_local, own)


def solution(mesh):
    def device_sweeps(data_local, start_block):
        chip_cols = start_block.shape[0] // 4
        row, col = lax.axis_index("row"), lax.axis_index("col")
        first, second = cut_of(chip_cols)
        base, core = (row * 2 + col // 2) * chip_cols, col % 2
        pieces = (lax.dynamic_slice_in_dim(start_block, base + core * (first // 2), first // 2), lax.dynamic_slice_in_dim(start_block, base + first + core * (second // 2), second // 2))
        low_rows = jnp.concatenate(pieces).astype(jnp.bfloat16)
        for _ in range(SWEEPS):
            q_rows, low_rows = sweep(data_local, low_rows)
        q_basis, ritz_vals = ritz(data_local, q_rows)
        return q_basis, ritz_vals.reshape(-1)

    return jax.shard_map(device_sweeps, mesh=mesh, in_specs=(P(("batch", "row", "col"), None), P("batch", None)), out_specs=(P("batch", None), P("batch")), check_vma=False)
```

```python
import jax
import jax.numpy as jnp
from jax import lax
from jax.experimental import pallas as pl
from jax.experimental.pallas import tpu as pltpu
from jax.sharding import PartitionSpec as P

SWEEPS = 4
ROW_CONTRACT = (((0,), (0,)), ((), ()))
LANE_CONTRACT = (((1,), (1,)), ((), ()))
PLAIN = (((1,), (0,)), ((), ()))
MESH = pl.DeviceIdType.MESH
HALF = 128
PEERS = 7
VMEM_BYTES = 63 * 1024 * 1024
TILES = 2
DEPTH = 3
TURNS = 8 * TILES
ROWS_AT_ONCE = 512


def exact_dot(left, right, dims):
    return lax.dot_general(left, right, dims, precision=lax.Precision.HIGHEST, preferred_element_type=jnp.float32)


def invert_factor(block):
    lane = lax.broadcasted_iota(jnp.int32, (8, HALF), 1)
    sub = lax.broadcasted_iota(jnp.int32, (8, HALF), 0)
    for step in range(HALF // 8):
        base = 8 * step
        inside = (lane >= base) & (lane < base + 8)
        pivots = block[base:base + 8, :]
        cols = [jnp.broadcast_to(pivots[:, base + p:base + p + 1], (8, HALF)) for p in range(8)]
        low = jnp.where(inside, jnp.where(lane - base == sub, 1.0, 0.0), pivots)
        full = low
        scale = jnp.zeros((8, HALF), jnp.float32)
        inverse = jnp.zeros((8, HALF), jnp.float32)
        for p in range(8):
            root = lax.rsqrt(jnp.broadcast_to(cols[p][p:p + 1, :], (8, HALF)))
            recip = root * root
            here = sub == p
            scale = jnp.where(here, root, scale)
            inverse = jnp.where(here, recip, inverse)
            mult = jnp.where(here, 0.0, cols[p] * recip)
            for q in range(p + 1, 8):
                cols[q] = cols[q] - mult * jnp.broadcast_to(cols[q][p:p + 1, :], (8, HALF))
            full_row = jnp.broadcast_to(full[p:p + 1, :], (8, HALF))
            low_row = jnp.broadcast_to(low[p:p + 1, :], (8, HALF))
            full = full - mult * full_row
            low = low - jnp.where(sub > p, mult, 0.0) * low_row
        block[base:base + 8, :] = low * scale
        full = full * inverse
        rows = [jnp.broadcast_to(full[p:p + 1, :], (8, HALF)) for p in range(8)]
        for i in range(step + 1, HALF // 8):
            held = block[8 * i:8 * i + 8, :]
            acc = jnp.where(inside, 0.0, held)
            for p in range(8):
                acc = acc - jnp.broadcast_to(held[:, base + p:base + p + 1], (8, HALF)) * rows[p]
            block[8 * i:8 * i + 8, :] = acc


def factor_inverse(gram, work, inv_low):
    tri = lax.broadcasted_iota(jnp.int32, (HALF, HALF), 0) >= lax.broadcasted_iota(jnp.int32, (HALF, HALF), 1)
    inv_low[:HALF, HALF:] = jnp.zeros((HALF, HALF), jnp.float32)

    @pl.loop(0, 2)
    def _(half):
        @pl.when(half == 0)
        def _():
            work[...] = gram[0:HALF, :]

        @pl.when(half == 1)
        def _():
            upper = exact_dot(inv_low[:HALF, :HALF], gram[HALF:2 * HALF, :], PLAIN)
            work[...] = gram[2 * HALF:3 * HALF, :] - exact_dot(upper, upper, ROW_CONTRACT)
            inv_low[HALF:, :HALF] = exact_dot(upper, inv_low[:HALF, :HALF], ROW_CONTRACT)

        invert_factor(work)
        block_inv = jnp.where(tri, work[...], 0.0)

        @pl.when(half == 0)
        def _():
            inv_low[:HALF, :HALF] = block_inv

        @pl.when(half == 1)
        def _():
            inv_low[HALF:, HALF:] = block_inv
            inv_low[HALF:, :HALF] = -exact_dot(block_inv, inv_low[HALF:, :HALF], PLAIN)


def orthonormalize(q_ref, low_ref, turned, part, slots, gram, work, inv_low, sum_send, sum_recv, out_send, out_recv):
    row, col = lax.axis_index("row"), lax.axis_index("col")
    me = row * 4 + col
    chunk = 3 * HALF // 8
    rows = turned.shape[1]

    def peer(offset):
        other = lax.rem(me + offset, 8)
        return (0, other // 4, lax.rem(other, 4)), other

    def share_gram(turn):
        mine = pl.ds(pl.multiple_of(me * chunk, 8), chunk)
        copies = []
        for offset in range(1, 8):
            device, other = peer(offset)
            copy = pltpu.make_async_remote_copy(
                src_ref=part.at[turn, pl.ds(pl.multiple_of(other * chunk, 8), chunk)],
                dst_ref=slots.at[turn, offset - 1],
                send_sem=sum_send.at[turn, offset - 1],
                recv_sem=sum_recv.at[turn, offset - 1],
                device_id=device,
                device_id_type=MESH,
            )
            copy.start()
            copies.append(copy)
        total = part[turn, mine, :]
        for offset in range(1, 8):
            copies[offset - 1].wait_recv()
            total = total + slots[turn, offset - 1]
        gram[turn, mine, :] = total
        spread = []
        for offset in range(1, 8):
            copy = pltpu.make_async_remote_copy(
                src_ref=gram.at[turn, mine],
                dst_ref=gram.at[turn, mine],
                send_sem=out_send.at[turn, offset - 1],
                recv_sem=out_recv.at[turn, offset - 1],
                device_id=peer(offset)[0],
                device_id_type=MESH,
            )
            copy.start()
            spread.append(copy)
        for copy in copies:
            copy.wait_send()
        for copy in spread:
            copy.wait()

    z_left, z_right = turned[:HALF, :].astype(jnp.bfloat16), turned[HALF:, :].astype(jnp.bfloat16)
    for place, (left, right) in enumerate(((z_left, z_left), (z_left, z_right), (z_right, z_right))):
        part[0, HALF * place:HALF * (place + 1), :] = lax.dot_general(left, right, LANE_CONTRACT, preferred_element_type=jnp.float32)

    def turn_body(turn):
        share_gram(turn)
        factor_inverse(gram.at[turn], work, inv_low)

        @pl.loop(0, rows // (2 * HALF))
        def _(i):
            block = pl.ds(pl.multiple_of(i * 2 * HALF, 2 * HALF), 2 * HALF)
            turned[:, block] = exact_dot(inv_low[...], turned[:, block], PLAIN)

        if rows % (2 * HALF):
            rest = pl.ds(rows // (2 * HALF) * 2 * HALF, HALF)
            turned[:, rest] = exact_dot(inv_low[...], turned[:, rest], PLAIN)

        @pl.when(turn == 0)
        def _():
            for place, (left, right) in enumerate(((0, 0), (0, HALF), (HALF, HALF))):
                part[1, HALF * place:HALF * (place + 1), :] = exact_dot(turned[left:left + HALF, :], turned[right:right + HALF, :], LANE_CONTRACT)

    pl.loop(0, 2)(turn_body)

    @pl.loop(0, rows // HALF)
    def _(i):
        block = pl.ds(pl.multiple_of(i * HALF, HALF), HALF)
        q_ref[block, :] = turned[:, block].T
        low_ref[block, :] = q_ref[block, :].astype(jnp.bfloat16)


def cut_of(chip_cols):
    first = 2 * HALF * ((chip_cols // (2 * HALF) + 1) // 2)
    return first, chip_cols - first


class Place:
    def __init__(self, features):
        self.row, self.col = lax.axis_index("row"), lax.axis_index("col")
        self.core, self.x = lax.rem(self.col, 2), self.col // 2
        self.twin = (0, self.row, self.col + 1 - 2 * self.core)
        self.x_side = (0, self.row, self.core + 2 * (1 - self.x))
        self.y_side = (0, 1 - self.row, self.col)
        self.chip_cols = features // 4
        self.widths = cut_of(self.chip_cols)

    def chip(self, flip_x, flip_y):
        x = self.x + flip_x - 2 * self.x * flip_x
        y = self.row + flip_y - 2 * self.row * flip_y
        return y * 2 + x

    def columns(self, flip_x, flip_y, sub):
        start = self.chip(flip_x, flip_y) * self.chip_cols + sub * self.widths[0]
        return pl.ds(pl.multiple_of(start, 2 * HALF), self.widths[sub])

    def owned(self, flip_x, flip_y, sub):
        start = self.chip(flip_x, flip_y) * self.chip_cols + sub * self.widths[0] + self.core * (self.widths[sub] // 2)
        return pl.ds(pl.multiple_of(start, HALF), self.widths[sub] // 2)


def as_int(flag):
    return jnp.where(flag, 1, 0)


def first_order(block):
    far = block >= 6
    in_x = (block == 2) | (block == 4) | far
    in_y = (block == 3) | (block == 5) | far
    return as_int(in_x), as_int(in_y), as_int((block == 1) | ((block >= 4) & (block <= 6)))


def second_order(block):
    far = block < 2
    in_x = far | (block == 3) | (block == 5)
    in_y = far | (block == 2) | (block == 4)
    return as_int(in_x), as_int(in_y), as_int((block == 1) | (block == 4) | (block == 5) | (block == 7))


def by_width(sub, action):
    for static in range(2):
        pl.when(sub == static)(lambda static=static: action(static))


def tile_copy(place, data, ring, ring_sem, tile, slot, order, begin):
    flip_x, flip_y, sub = order(tile // TILES)
    tile_rows = ring.shape[1]
    rows = pl.ds(pl.multiple_of(lax.rem(tile, TILES) * tile_rows, tile_rows), tile_rows)

    def act(static):
        copy = pltpu.make_async_copy(data.at[rows, place.columns(flip_x, flip_y, static)], ring.at[slot, :, pl.ds(0, place.widths[static])], ring_sem.at[slot])
        copy.start() if begin else copy.wait()

    by_width(sub, act)


def open_ring(place, data, ring, ring_sem):
    for turn in range(DEPTH):
        tile_copy(place, data, ring, ring_sem, turn, turn, first_order, True)


def meet(place):
    barrier = pltpu.get_barrier_semaphore()
    for offset in range(1, 8):
        other = lax.rem(place.row * 4 + place.col + offset, 8)
        pl.semaphore_signal(barrier, inc=1, device_id=(0, other // 4, lax.rem(other, 4)), device_id_type=MESH)
    pl.semaphore_wait(barrier, PEERS)


def first_pass(place, data, own, landing, basis, ring, acc, ring_sem, gather_sem, second, clear, finish, after):
    turns = TURNS
    tile_rows = ring.shape[1]
    piece = (pl.ds(0, place.widths[0] // 2), pl.ds(place.widths[0] // 2, place.widths[1] // 2))

    def hand(index, flip_x, flip_y, sub, device):
        rows = place.owned(flip_x, flip_y, sub)
        source = own.at[piece[sub]] if flip_x + flip_y == 0 else landing.at[rows]
        return pltpu.make_async_remote_copy(
            src_ref=source, dst_ref=landing.at[rows], send_sem=gather_sem.at[0, index], recv_sem=gather_sem.at[1, index], device_id=device, device_id_type=MESH
        )

    twin, x_side, y_side = place.twin, place.x_side, place.y_side
    copies = [
        hand(0, 0, 0, 0, x_side), hand(1, 0, 0, 0, y_side), hand(2, 0, 0, 0, twin),
        hand(3, 0, 0, 1, x_side), hand(4, 0, 0, 1, y_side), hand(5, 0, 0, 1, twin),
        hand(6, 1, 0, 0, y_side), hand(7, 1, 0, 0, twin), hand(8, 1, 0, 1, twin),
        hand(9, 0, 1, 1, x_side), hand(10, 0, 1, 0, twin), hand(11, 0, 1, 1, twin),
        hand(12, 1, 1, 0, twin), hand(13, 1, 1, 1, twin),
    ]
    for index in range(6):
        copies[index].start()
    for sub in range(2):
        landing[place.owned(0, 0, sub), :] = own[piece[sub], :]
    acc[...] = jnp.zeros_like(acc)
    clear()

    def at(turn, when, waits, starts):
        @pl.when(turn == when)
        def _():
            for index in waits:
                copies[index].wait_recv()
            for index in starts:
                copies[index].start()

    @pl.loop(0, turns)
    def _(turn):
        at(turn, 0, (2,), ())
        at(turn, TILES, (5,), ())
        at(turn, 2 * TILES - 1, (0,), (6, 7))
        at(turn, 2 * TILES - 1, (1,), (10,))
        at(turn, 2 * TILES, (7,), ())
        at(turn, 3 * TILES, (10,), ())
        at(turn, 3 * TILES + TILES // 2, (3, 4), (8, 9, 11))
        at(turn, 4 * TILES, (8,), ())
        at(turn, 5 * TILES, (11,), ())
        at(turn, 6 * TILES - 1, (9, 6), (13, 12))
        at(turn, 6 * TILES, (13,), ())
        at(turn, 7 * TILES, (12,), ())
        slot = lax.rem(turn, DEPTH)
        flip_x, flip_y, sub = first_order(turn // TILES)
        tile_copy(place, data, ring, ring_sem, turn, slot, first_order, False)
        part_rows = min(ROWS_AT_ONCE, tile_rows)

        def project(static):
            cols = place.columns(flip_x, flip_y, static)
            if landing is not basis:
                @pl.when(lax.rem(turn, TILES) == 0)
                def _():
                    basis[cols, :] = landing[cols, :].astype(jnp.bfloat16)
            for half in range(tile_rows // part_rows):
                inner = pl.ds(half * part_rows, part_rows)
                rows = pl.ds(pl.multiple_of(lax.rem(turn, TILES) * tile_rows + half * part_rows, part_rows), part_rows)
                acc[rows, :] += jnp.dot(ring[slot, inner, pl.ds(0, place.widths[static])], basis[cols, :], preferred_element_type=jnp.float32)

        by_width(sub, project)

        @pl.when(turn + DEPTH < turns)
        def _():
            tile_copy(place, data, ring, ring_sem, turn + DEPTH, slot, first_order, True)

        if second is not None:
            @pl.when((turn + DEPTH >= turns) & (turn < turns - TILES))
            def _():
                tile_copy(place, data, ring, ring_sem, turn + DEPTH - (turns - TILES), slot, second, True)

        @pl.when(turn >= turns - TILES)
        def _():
            tile = lax.rem(turn, TILES)
            finish(tile, acc[pl.ds(pl.multiple_of(tile * tile_rows, tile_rows), tile_rows), :])

    after()
    for copy in copies:
        copy.wait_send()


def sweep_kernel(data, own, q_ref, low, turned, gram_part, gram_slots, gram, work, inv_low, sum_send, sum_recv, out_send, out_recv, basis, ring, acc, proj_t, part0, part1, twin0, twin1, far0, far1, side0, side1, ring_sem, gather_sem, twin_sem, far_sem, side_sem):
    place = Place(data.shape[1])
    open_ring(place, data, ring, ring_sem)
    low[...] = own[...]
    meet(place)

    @pl.loop(0, SWEEPS)
    def _(sweep_index):
        twin, x_side, y_side = place.twin, place.x_side, place.y_side
        part, from_twin, from_far, from_side = (part0, part1), (twin0, twin1), (far0, far1), (side0, side1)
        halves = tuple(width // 2 for width in place.widths)
        width = turned.shape[0]
        top = width // 2
        turns = TURNS

        def clear():
            part0[...] = jnp.zeros_like(part0)
            part1[...] = jnp.zeros_like(part1)

        def finish(tile, rows):
            proj_t[tile] = rows.astype(jnp.bfloat16).T

        first_pass(place, data, low, basis, basis, ring, acc, ring_sem, gather_sem, second_order, clear, finish, lambda: None)

        upper, lower = pl.ds(0, top), pl.ds(top, width - top)
        mine = tuple(pl.ds(pl.multiple_of(place.core * half, HALF), half) for half in halves)
        other = tuple(pl.ds(pl.multiple_of((1 - place.core) * half, HALF), half) for half in halves)
        FAR, Y, X, OWN = 0, 1, 2, 3

        def remote(source, target, sems, device):
            return pltpu.make_async_remote_copy(src_ref=source, dst_ref=target, send_sem=sems.at[0], recv_sem=sems.at[1], device_id=device, device_id_type=MESH)

        swaps, relays, delivers = {}, {}, {}
        for sub in range(2):
            for kind in range(4):
                swaps[kind, sub] = remote(part[sub].at[kind, :, other[sub]], from_twin[sub].at[kind], twin_sem.at[kind, sub], twin)
            relays[0, sub] = remote(part[sub].at[FAR, upper, mine[sub]], from_far[sub].at[0], far_sem.at[0, sub], x_side)
            relays[1, sub] = remote(part[sub].at[FAR, lower, mine[sub]], from_far[sub].at[1], far_sem.at[1, sub], y_side)
            for kind, device in ((Y, y_side), (X, x_side)):
                for which, rows in ((0, upper), (1, lower)):
                    delivers[kind, which, sub] = remote(part[sub].at[kind, rows, mine[sub]], from_side[sub].at[kind - 1, rows], side_sem.at[kind - 1, which, sub], device)

        def lift(kind, sub):
            swaps[kind, sub].wait_recv()
            part[sub][kind, :, mine[sub]] = part[sub][kind, :, mine[sub]] + from_twin[sub][kind]

        def send_far(sub):
            lift(FAR, sub)
            relays[0, sub].start()
            relays[1, sub].start()

        def send_side(kind, sub):
            lift(kind, sub)
            plain, joined, rows = (1, 0, upper) if kind == Y else (0, 1, lower)
            delivers[kind, plain, sub].start()
            relays[joined, sub].wait_recv()
            part[sub][kind, rows, mine[sub]] = part[sub][kind, rows, mine[sub]] + from_far[sub][joined]
            delivers[kind, joined, sub].start()

        order = ((FAR, 0), (FAR, 1), (Y, 0), (X, 0), (Y, 1), (X, 1), (OWN, 0), (OWN, 1))

        @pl.loop(0, turns)
        def _(turn):
            slot = lax.rem(turn + turns - TILES, DEPTH)
            block, tile = turn // TILES, lax.rem(turn, TILES)
            sub = second_order(block)[2]

            @pl.when(turn >= TILES)
            def _():
                tile_copy(place, data, ring, ring_sem, turn, slot, second_order, False)

            kind = jnp.where(block < 2, FAR, jnp.where(block >= 6, OWN, jnp.where((block == 2) | (block == 4), Y, X)))

            def pull(static):
                part[static][kind] += jnp.dot(proj_t[tile], ring[slot, :, pl.ds(0, place.widths[static])], preferred_element_type=jnp.float32)

            by_width(sub, pull)

            @pl.when(turn + DEPTH < turns)
            def _():
                tile_copy(place, data, ring, ring_sem, turn + DEPTH, slot, second_order, True)

            for index, (held, held_sub) in enumerate(order):
                pl.when(turn == (index + 1) * TILES - 1)(lambda held=held, held_sub=held_sub: swaps[held, held_sub].start())
                if held == FAR:
                    pl.when(turn == (index + 1) * TILES + 0)(lambda held_sub=held_sub: send_far(held_sub))
                elif held != OWN:
                    pl.when(turn == (index + 1) * TILES + 0)(lambda held=held, held_sub=held_sub: send_side(held, held_sub))

        for sub in range(2):
            lanes = pl.ds(sub * halves[0], halves[sub])
            lift(OWN, sub)
            for kind in (Y, X):
                for which in range(2):
                    delivers[kind, which, sub].wait_recv()
            turned[:, lanes] = (part[sub][OWN, :, mine[sub]] + from_side[sub][0]) + from_side[sub][1]
        @pl.when(sweep_index < SWEEPS - 1)
        def _():
            open_ring(place, data, ring, ring_sem)

        orthonormalize(q_ref, low, turned, gram_part, gram_slots, gram, work, inv_low, sum_send, sum_recv, out_send, out_recv)
        for copy in (*swaps.values(), *relays.values(), *delivers.values()):
            copy.wait_send()


def ritz_kernel(data, own, q_ref, r_ref, basis, ring, acc, slots, ring_sem, gather_sem, share_sem):
    place = Place(data.shape[1])
    me = place.row * 4 + place.col
    width = q_ref.shape[1]

    def clear():
        slots[me] = jnp.zeros((8, width), jnp.float32)

    def finish(tile, rows):
        slots[me] += jnp.sum((rows * rows).reshape(rows.shape[0] // 8, 8, width), axis=0)

    def after():
        sends = []
        for offset in range(1, 8):
            other = lax.rem(me + offset, 8)
            copy = pltpu.make_async_remote_copy(
                src_ref=slots.at[me], dst_ref=slots.at[me], send_sem=share_sem.at[0, offset - 1], recv_sem=share_sem.at[1, offset - 1],
                device_id=(0, other // 4, lax.rem(other, 4)), device_id_type=MESH,
            )
            copy.start()
            sends.append(copy)
        for copy in sends:
            copy.wait()
        total = slots[0]
        for index in range(1, 8):
            total = total + slots[index]
        r_ref[...] = jnp.sum(total, axis=0, keepdims=True)

    open_ring(place, data, ring, ring_sem)
    meet(place)
    first_pass(place, data, own, q_ref, basis, ring, acc, ring_sem, gather_sem, None, clear, finish, after)


def stream_scratch(rows, features, width):
    return [
        pltpu.VMEM((features, width), jnp.bfloat16),
        pltpu.VMEM((DEPTH, rows // TILES, cut_of(features // 4)[0]), jnp.bfloat16),
        pltpu.VMEM((rows, width), jnp.float32),
    ]


def sweeps(data_local, own):
    rows, features = data_local.shape
    width = own.shape[1]
    widths = cut_of(features // 4)
    pairs = []
    for shape in ((4, width), (4, width), (2, width // 2), (2, width)):
        scale = 1 if not pairs else 2
        pairs += [pltpu.VMEM((*shape, size // scale), jnp.float32) for size in widths]
    return pl.pallas_call(
        sweep_kernel,
        out_shape=jax.ShapeDtypeStruct((features // 8, width), jnp.float32),
        in_specs=[pl.BlockSpec(memory_space=pl.ANY), pl.BlockSpec(memory_space=pltpu.VMEM)],
        out_specs=pl.BlockSpec(memory_space=pltpu.VMEM),
        scratch_shapes=[
            pltpu.VMEM((features // 8, width), jnp.bfloat16),
            pltpu.VMEM((width, features // 8), jnp.float32),
            pltpu.VMEM((2, 3 * HALF, HALF), jnp.float32),
            pltpu.VMEM((2, PEERS, 3 * HALF // 8, HALF), jnp.float32),
            pltpu.VMEM((2, 3 * HALF, HALF), jnp.float32),
            pltpu.VMEM((HALF, HALF), jnp.float32),
            pltpu.VMEM((2 * HALF, 2 * HALF), jnp.float32),
            pltpu.SemaphoreType.DMA((2, PEERS)),
            pltpu.SemaphoreType.DMA((2, PEERS)),
            pltpu.SemaphoreType.DMA((2, PEERS)),
            pltpu.SemaphoreType.DMA((2, PEERS)),
            *stream_scratch(rows, features, width),
            pltpu.VMEM((TILES, width, rows // TILES), jnp.bfloat16),
            *pairs,
            pltpu.SemaphoreType.DMA((DEPTH,)),
            pltpu.SemaphoreType.DMA((2, 14)),
            pltpu.SemaphoreType.DMA((4, 2, 2)),
            pltpu.SemaphoreType.DMA((2, 2, 2)),
            pltpu.SemaphoreType.DMA((2, 2, 2, 2)),
        ],
        compiler_params=pltpu.CompilerParams(collective_id=1, has_side_effects=True, vmem_limit_bytes=VMEM_BYTES),
        cost_estimate=pl.CostEstimate(flops=16 * rows * features * width, bytes_accessed=16 * rows * features, transcendentals=0),
        name="sweeps",
    )(data_local, own)


def ritz(data_local, own):
    rows, features = data_local.shape
    width = own.shape[1]
    return pl.pallas_call(
        ritz_kernel,
        out_shape=(jax.ShapeDtypeStruct((features, width), jnp.float32), jax.ShapeDtypeStruct((1, width), jnp.float32)),
        in_specs=[pl.BlockSpec(memory_space=pl.ANY), pl.BlockSpec(memory_space=pltpu.VMEM)],
        out_specs=(pl.BlockSpec(memory_space=pltpu.VMEM), pl.BlockSpec(memory_space=pltpu.VMEM)),
        scratch_shapes=[
            *stream_scratch(rows, features, width),
            pltpu.VMEM((8, 8, width), jnp.float32),
            pltpu.SemaphoreType.DMA((DEPTH,)),
            pltpu.SemaphoreType.DMA((2, 14)),
            pltpu.SemaphoreType.DMA((2, 7)),
        ],
        compiler_params=pltpu.CompilerParams(collective_id=2, has_side_effects=True, vmem_limit_bytes=VMEM_BYTES),
        cost_estimate=pl.CostEstimate(flops=2 * rows * features * width, bytes_accessed=2 * rows * features, transcendentals=0),
        name="ritz",
    )(data_local, own)


def solution(mesh):
    def device_sweeps(data_local, start_block):
        chip_cols = start_block.shape[0] // 4
        row, col = lax.axis_index("row"), lax.axis_index("col")
        first, second = cut_of(chip_cols)
        base, core = (row * 2 + col // 2) * chip_cols, col % 2
        pieces = (lax.dynamic_slice_in_dim(start_block, base + core * (first // 2), first // 2), lax.dynamic_slice_in_dim(start_block, base + first + core * (second // 2), second // 2))
        low_rows = jnp.concatenate(pieces).astype(jnp.bfloat16)
        q_basis, ritz_vals = ritz(data_local, sweeps(data_local, low_rows))
        return q_basis, ritz_vals.reshape(-1)

    return jax.shard_map(device_sweeps, mesh=mesh, in_specs=(P(("batch", "row", "col"), None), P("batch", None)), out_specs=(P("batch", None), P("batch")), check_vma=False)
```
